32 devices in a mesh: grp: 8 (over y, x, core), col: 4 (over z).
Axes of the slice: x: 2, y: 2, z: 4, core: 2. Of those that a mesh axis runs over, the one named last changes fastest.
Arguments:
- old_tables: bfloat16 [32, 128, 32768], P(('grp', 'col')), may hold values from -3 to 3
- table_rows: int32 [32], replicated, may hold values from 4096 to 32768, as said below
- old_plan: int32 [32], replicated, may hold values from 0 to 31, each once
- new_plan: int32 [32], replicated, may hold values from 0 to 31, each once
- ids: int32 [256, 32, 16], P(('grp', 'col')), may hold values from 0 to 32767, as said below
- bag_len: int32 [256, 32], P(('grp', 'col')), may hold values from 1 to 16
Outputs:
- new_tables: bfloat16 [32, 128, 32768], P('grp', 'col')
- pooled: float32 [256, 32, 128], P(('grp', 'col'))
The draws below stay inside these ranges and needn't reach their ends.
Inputs may be any that keep to these rules, and one draw needn't show every extreme that they name: table_rows[t] is a multiple of 4096, and some table has exactly 32768 rows. `ids`: every id of table t lies below table_rows[t].
All inputs are finite; a program needn't handle non-finite values.
Results may differ from the reference program's by a relative error of at most 0.001.
Values may be sent and summed in bfloat16 or wider, within the bound.
A program may use at most 128 MiB of HBM per device.

```python
import jax
import jax.numpy as jnp
from jax import lax

W = 128
ROWS = 32768
BAG = 16
TABLES = 32
BATCH = 256


def table_sizes(key):
    base = jax.random.fold_in(key, 7)
    eighths = jax.random.randint(jax.random.fold_in(base, 1), (TABLES,), 1, 9)
    chosen = jax.random.randint(jax.random.fold_in(base, 2), (), 0, TABLES)
    eighths = jnp.where(jnp.arange(TABLES) == chosen, 8, eighths)
    return (eighths * (ROWS // 8)).astype(jnp.int32)


def draw_table_rows(key, part):
    return table_sizes(key)


def draw_ids(key, part):
    limits = table_sizes(key)
    drawn = jax.random.randint(jax.random.fold_in(key, 11), (BATCH, TABLES, BAG), 0, limits[None, :, None])
    return drawn.astype(jnp.int32)


def with_ends(values, own_key, low, largest):
    longest = values.shape.index(max(values.shape))
    spots = []
    for shift in (0, 1):
        where = [jax.random.randint(jax.random.fold_in(own_key, axis), (), 0, length) for axis, length in enumerate(values.shape)]
        where[longest] = (where[longest] + shift) % values.shape[longest]
        spots.append(tuple(where))
    return values.at[spots[0]].set(low).at[spots[1]].set(largest)


def shard_levels(key, dims, shards, smallest, largest):
    def one(dim, parts):
        heights = jax.random.uniform(jax.random.fold_in(jax.random.fold_in(key, 6), dim), (parts,), jnp.float32, smallest / len(shards), largest / len(shards))
        return jnp.repeat(jnp.exp(heights), dims[dim] // parts).reshape((-1,) + (1,) * (len(dims) - dim - 1))

    loudness = one(*shards[0])
    for cut in shards[1:]:
        loudness = loudness * one(*cut)
    return loudness


def centred(stream_key, shape, spread, bound, cuts=(), held_as=jnp.bfloat16):
    result = jax.random.normal(stream_key, shape, jnp.float32) * spread
    if len(cuts) > 0:
        result = shard_levels(stream_key, shape, cuts, -0.22, 0.18) * result
    return jnp.clip(result, min=-bound, max=bound).astype(held_as)


def setup_inputs(seed: int = 0) -> dict:
    splits = jax.random.split(jax.random.key(seed), 7)
    return {
        "old_tables": centred(splits[0], (TABLES, W, ROWS), 0.5, 3.0, ((0, 32),)),
        "table_rows": draw_table_rows(jax.random.fold_in(splits[6], 71), 0),
        "old_plan": jax.random.permutation(splits[2], TABLES).astype(jnp.int32),
        "new_plan": jax.random.permutation(splits[3], TABLES).astype(jnp.int32),
        "ids": draw_ids(jax.random.fold_in(splits[6], 71), 0),
        "bag_len": with_ends(jax.random.randint(splits[5], (BATCH, TABLES), 1, BAG + 1), jax.random.fold_in(splits[5], 1), 1, BAG).astype(jnp.int32),
    }


def reference(old_tables, table_rows, old_plan, new_plan, ids, bag_len):
    old_inverse = jnp.argsort(old_plan).astype(jnp.int32)
    new_inverse = jnp.argsort(new_plan).astype(jnp.int32)
    row_iota = jnp.arange(ROWS, dtype=jnp.int32)
    bag_iota = jnp.arange(BAG, dtype=jnp.int32)

    def one_table(position):
        table_id = new_plan[position]
        old_slot = old_inverse[table_id]
        stored = lax.dynamic_index_in_dim(old_tables, old_slot, 0, keepdims=False)
        keep_rows = (row_iota < table_rows[table_id]).astype(old_tables.dtype)
        masked = stored * keep_rows[None, :]
        table_ids = lax.dynamic_index_in_dim(ids, table_id, 1, keepdims=False)
        lengths = lax.dynamic_index_in_dim(bag_len, table_id, 1, keepdims=False)
        values = jnp.take(masked, table_ids, axis=1).astype(jnp.float32)
        in_bag = (bag_iota[None, :] < lengths[:, None]).astype(jnp.float32)
        sums = jnp.sum(values * in_bag[None, :, :], axis=2)
        return masked, sums

    new_tables, sums = lax.map(one_table, jnp.arange(TABLES, dtype=jnp.int32))
    pooled = jnp.transpose(sums[new_inverse], (2, 0, 1))
    return new_tables, pooled
```

```python
import functools

import jax
import jax.numpy as jnp
from jax import lax
from jax.experimental import pallas as pl
from jax.experimental.pallas import tpu as pltpu
from jax.sharding import PartitionSpec as P

UNIT = 4096
LANES = 128
NARROW = 16
MESH = pl.DeviceIdType.MESH
AHEAD = 2
WINDOW = 2
CHUNKS = 32
ORDER = (4, 2, 6, 3, 5, 7, 1)
VMEM_ROOM = 56 * 1024 * 1024
LAG = 2
SHARES = (10, 11, 12, 13, 16)


def chunk_list(unit, halves):
    chunks = []
    for start in range(0, unit, 8 * LANES):
        for half in range(halves):
            chunks.append((1, 4, half, start))
    return chunks


def move_kernel(shape, chunks, caps, old_ref, new_ref, table_ref, ids_ref, pick_ref, out_ref, pooled_ref, *scratch):
    groups, cols, units, width, per_group = shape
    count = len(chunks)
    spread, planes, gathered = scratch[:count], scratch[count : 2 * count], scratch[2 * count : 3 * count]
    (abuf, zbuf, cbuf, fbuf, a_send, a_recv, z_send, z_recv, c_send, c_recv, f_send, f_recv,
     own_ids, by_slot, held_ref, total, sums_ref, source_ref, inverse_ref,
     i_send, i_recv, r_send, r_recv, t_sem) = scratch[3 * count :]
    g = lax.axis_index("grp")
    c = lax.axis_index("col")
    chip, core = g // 2, lax.rem(g, 2)
    chips = groups // 2
    cw = spread[0].shape[2]
    devices = groups * cols
    me = g * cols + c
    samples, tables, bag = ids_ref.shape
    slots, room = caps

    def aligned(value, unit):
        return pl.multiple_of(value * unit, unit)

    def place(k):
        stride, over, half, start = chunks[k]
        return stride, over, half, start, lax.rem(chip // stride, over)

    def spread_to(k, d):
        stride, over, half, start, mine = place(k)
        to_core = lax.rem(core + d // over, 2)
        to_part = lax.rem(mine + d % over, over)
        return to_core, to_part, (chip + (to_part - mine) * stride) * 2 + to_core

    def spread_step(k, d):
        stride, over, half, start, mine = place(k)
        slot = core * over + mine
        return pltpu.make_async_remote_copy(
            abuf.at[k % 2, d], spread[k].at[pl.ds(slot * units, units)], a_send.at[k, d], a_recv.at[k, d],
            device_id=(spread_to(k, d)[2], c), device_id_type=MESH,
        )

    def spread_start(k):
        stride, over, half, start, mine = place(k)
        slot = core * over + mine
        if k >= 2:
            for d in range(1, 2 * over):
                spread_step(k - 2, d).wait_send()
        for d in list(range(1, 2 * over)) + [0]:
            to_core, to_part, to = spread_to(k, d)
            block = start // LANES + to_core * over + to_part

            def step(e, carry):
                rows = pl.ds(aligned(e * (UNIT // LANES) + block, LANES), LANES)
                if d == 0:
                    spread[k][slot * units + e] = held_ref[:, half, :, rows]
                else:
                    abuf[k % 2, d, e] = held_ref[:, half, :, rows]
                return carry

            lax.fori_loop(0, units, step, 0, unroll=2)
            if d > 0:
                spread_step(k, d).start()

    def column_step(k, d):
        to = lax.rem(c + d, cols)
        return pltpu.make_async_remote_copy(
            zbuf.at[k % 2, to], planes[k].at[pl.ds(c * slots, slots)], z_send.at[k, d], z_recv.at[k, d],
            device_id=(g, to), device_id_type=MESH,
        )

    def chip_step(k, d):
        to = lax.rem(chip + d, chips)
        return pltpu.make_async_remote_copy(
            cbuf.at[k % 2, d], gathered[k].at[pl.ds(chip * room, room)], c_send.at[k, d], c_recv.at[k, d],
            device_id=(to * 2 + core, c), device_id_type=MESH,
        )

    def out_start(k):
        stride, over, half, start, mine = place(k)
        rows = over * LANES
        for d in (1, 0):

            def step(e, carry):
                src = fbuf.at[k % 2, d, e]
                dst = out_ref.at[
                    :, pl.ds(half * cw, cw),
                    pl.ds(aligned(e * (UNIT // LANES) + start // LANES + core * over, LANES), rows),
                ]
                if d == 0:
                    pltpu.make_async_copy(src, dst, f_recv.at[k, 0]).start()
                else:
                    pltpu.make_async_remote_copy(
                        src, dst, f_send.at[k], f_recv.at[k, 1],
                        device_id=(chip * 2 + lax.rem(core + 1, 2), c), device_id_type=MESH,
                    ).start()
                return carry

            lax.fori_loop(0, units, step, 0)

    def out_done(k, d):
        part = fbuf.at[k % 2, d]
        if d == 0:
            return pltpu.make_async_copy(part, part, f_recv.at[k, 0])
        return pltpu.make_async_remote_copy(
            part, part, f_send.at[k], f_recv.at[k, 1],
            device_id=(chip * 2 + lax.rem(core + 1, 2), c), device_id_type=MESH,
        )

    def ids_step(d):
        to = lax.rem(me + d, devices)
        src, dst = by_slot.at[to], own_ids.at[me]
        if isinstance(d, int):
            return pltpu.make_async_copy(src, dst, i_recv.at[d])
        return pltpu.make_async_remote_copy(
            src, dst, i_send.at[d], i_recv.at[d],
            device_id=(to // cols, lax.rem(to, cols)), device_id_type=MESH,
        )

    def sums_step(d):
        to = lax.rem(me + d, devices)
        src, dst = total.at[to], sums_ref.at[me]
        if isinstance(d, int):
            return pltpu.make_async_copy(src, dst, r_recv.at[d])
        return pltpu.make_async_remote_copy(
            src, dst, r_send.at[d], r_recv.at[d],
            device_id=(to // cols, lax.rem(to, cols)), device_id_type=MESH,
        )

    def each_peer(act):
        def step(d, carry):
            act(d)
            return carry

        lax.fori_loop(1, devices, step, 0)

    piece_rows = 1024
    pieces = units * UNIT // piece_rows

    def fetch(e):
        rows = pl.ds(aligned(e, UNIT), UNIT)
        return pltpu.make_async_copy(table_ref.at[:, :, :, rows], held_ref.at[:, :, :, rows], t_sem.at[e])

    tile = 512 if piece_rows % 512 == 0 else 128
    fold = 8 if devices % 8 == 0 else 1

    def pool(first, last):
        def one(j, carry):
            columns = piece_rows // tile

            def piece(step, carry):
                block, part = step // columns, lax.rem(step, columns)
                rows = samples * fold
                wanted = own_ids[pl.ds(block * fold, fold)].reshape(rows, bag)
                row = lax.broadcasted_iota(jnp.int32, (rows, tile), 1) + (j * piece_rows + part * tile)
                counts = jnp.zeros((rows, tile), jnp.float32)
                for i in range(bag):
                    counts = jnp.where(wanted[:, i : i + 1] == row, counts + 1.0, counts)
                values = held_ref[:, :, :, pl.ds(aligned(j * columns + part, tile), tile)].reshape(width, tile)
                sums = lax.dot_general(
                    counts.astype(values.dtype), values, (((1,), (1,)), ((), ())),
                    preferred_element_type=jnp.float32,
                )
                where = pl.ds(block * fold, fold)
                total[where] = total[where] + sums.reshape(fold, samples, width)
                return carry

            lax.fori_loop(0, devices // fold * columns, piece, 0)
            return carry

        lax.fori_loop(first, last, one, 0)

    def order_ids(s, carry):
        by_slot[s] = ids_ref[:, pl.ds(old_ref[s], 1), :].reshape(samples, bag)
        return carry

    def locate(j, carry):
        def look(s, found):
            return jnp.where(old_ref[s] == j, s, found)

        inverse_ref[j] = lax.fori_loop(0, tables, look, 0)
        return carry

    c_base = slots
    f_base = slots + chips * room

    def pack_columns(k):
        for d in range(1, 2 * chunks[k][1]):
            spread_step(k, d).wait_recv()
        if k >= 2:
            for d in range(1, cols):
                column_step(k - 2, d).wait_send()

        def one(n, carry):
            item = pick_ref[n]
            for z in range(cols):
                zbuf[k % 2, z, n] = spread[k][item, z]
            planes[k][c * slots + n] = spread[k][item, c]
            return carry

        lax.fori_loop(0, slots, one, 0)
        for d in COLUMN_ORDER(cols):
            column_step(k, d).start()

    def pack_chips(k):
        for d in range(1, cols):
            column_step(k, d).wait_recv()
        if k >= 2:
            for d in range(1, chips):
                chip_step(k - 2, d).wait_send()
        for d in list(range(1, chips)) + [0]:

            def one(m, carry):
                item = planes[k][pick_ref[c_base + d * room + m]]
                if d == 0:
                    gathered[k][chip * room + m] = item
                else:
                    cbuf[k % 2, d, m] = item
                return carry

            lax.fori_loop(0, room, one, 0, unroll=4)
            if d > 0:
                chip_step(k, d).start()

    def finish(k):
        stride, over, half, start, mine = place(k)
        for d in range(1, chips):
            chip_step(k, d).wait_recv()
        if k >= 2:
            out_done(k - 2, 0).wait()
            out_done(k - 2, 1).wait_send()
        for d in range(2):
            owner = lax.rem(core + d, 2)

            def one(e, carry):
                for j in range(per_group):
                    item = pick_ref[f_base + (owner * per_group + j) * units + e]
                    for b in range(over):
                        fbuf[k % 2, d, e, j, :, b * LANES : (b + 1) * LANES] = gathered[k][item + b * stride * room]
                return carry

            lax.fori_loop(0, units, one, 0)
        out_start(k)

    for e in range(units):
        fetch(e).start()
    lax.fori_loop(0, tables, order_ids, 0)
    for e in range(units):
        fetch(e).wait()
    for k in range(min(AHEAD, count)):
        spread_start(k)
    each_peer(lambda d: ids_step(d).start())
    ids_step(0).start()
    total[...] = jnp.zeros_like(total)
    lax.fori_loop(0, tables, locate, 0)
    each_peer(lambda d: ids_step(d).wait_recv())
    ids_step(0).wait()

    steps = count + 1
    share = -(-pieces // steps)
    used = 0
    for t in range(count + LAG + 1):
        if t < count:
            pack_columns(t)
            if t + AHEAD < count:
                spread_start(t + AHEAD)
        if used < pieces:
            last = min(used + share, pieces)
            pool(used, last)
            used = last
            if used == pieces:
                each_peer(lambda d: sums_step(d).start())
                sums_step(0).start()
        if 1 <= t <= count:
            pack_chips(t - 1)
        if t >= LAG + 1:
            finish(t - LAG - 1)
    for k in range(count):
        out_done(k, 1).wait_recv()
    for k in range(max(count - 2, 0), count):
        for d in range(1, 2 * chunks[k][1]):
            spread_step(k, d).wait_send()
        for d in range(1, cols):
            column_step(k, d).wait_send()
        for d in range(1, chips):
            chip_step(k, d).wait_send()
        out_done(k, 0).wait()
        out_done(k, 1).wait_send()
    each_peer(lambda d: ids_step(d).wait_send())
    each_peer(lambda d: sums_step(d).wait())
    sums_step(0).wait()
    for t in range(tables):
        pooled_ref[:, t, :] = sums_ref[inverse_ref[t]]


def COLUMN_ORDER(cols):
    return [d for d in (2, 1, 3) if d < cols] + list(range(4, cols))


def move_tables(old_tables, old_plan, new_plan, marked, picks, groups, cols, chunks, caps):
    _, width, table_len = old_tables.shape
    narrow = width // cols
    halves = narrow // NARROW
    tables = old_plan.shape[0]
    per_group = tables // groups
    units = table_len // UNIT
    count = len(chunks)
    dtype = old_tables.dtype
    devices = groups * cols
    chips = groups // 2
    samples, _, bag = marked.shape
    slots, room = caps
    tile = (NARROW, LANES)
    over = max(chunk[1] for chunk in chunks)
    dma = pltpu.SemaphoreType.DMA
    view = old_tables.reshape(cols, halves, NARROW, table_len)
    return pl.pallas_call(
        functools.partial(move_kernel, (groups, cols, units, width, per_group), chunks, caps),
        out_shape=(
            jax.ShapeDtypeStruct((per_group, narrow, table_len), dtype),
            jax.ShapeDtypeStruct((samples, tables, width), jnp.float32),
        ),
        in_specs=[
            pl.BlockSpec(memory_space=pltpu.SMEM),
            pl.BlockSpec(memory_space=pltpu.SMEM),
            pl.BlockSpec(memory_space=pl.ANY),
            pl.BlockSpec(memory_space=pltpu.VMEM),
            pl.BlockSpec(memory_space=pltpu.SMEM),
        ],
        out_specs=(pl.BlockSpec(memory_space=pl.ANY), pl.BlockSpec(memory_space=pltpu.VMEM)),
        scratch_shapes=[pltpu.VMEM((2 * chunk[1] * units, cols) + tile, dtype) for chunk in chunks]
        + [pltpu.VMEM((cols * slots,) + tile, dtype)] * count
        + [pltpu.VMEM((chips * room,) + tile, dtype)] * count
        + [
            pltpu.VMEM((2, 2 * over, units, cols) + tile, dtype),
            pltpu.VMEM((2, cols, slots) + tile, dtype),
            pltpu.VMEM((2, chips, room) + tile, dtype),
            pltpu.VMEM((2, 2, units, per_group, NARROW, over * LANES), dtype),
            dma((count, 2 * over)), dma((count, 2 * over)),
            dma((count, cols)), dma((count, cols)),
            dma((count, chips)), dma((count, chips)),
            dma((count,)), dma((count, 2)),
            pltpu.VMEM((devices, samples, bag), marked.dtype),
            pltpu.VMEM((devices, samples, bag), marked.dtype),
            pltpu.VMEM((cols, halves, NARROW, table_len), dtype),
            pltpu.VMEM((devices, samples, width), jnp.float32),
            pltpu.VMEM((devices, samples, width), jnp.float32),
            pltpu.SMEM((tables,), jnp.int32),
            pltpu.SMEM((tables,), jnp.int32),
        ]
        + [dma((devices,))] * 4
        + [dma((units,))],
        compiler_params=pltpu.CompilerParams(
            has_side_effects=True, vmem_limit_bytes=60 * 1024 * 1024
        ),
    )(old_plan, new_plan, view, marked, picks)


def whole_kernel(groups, cols, chunks, old_ref, new_ref, table_ref, ids_ref, out_ref, pooled_ref, *scratch):
    zbufs, spreads, picks = scratch[:chunks], scratch[chunks : 2 * chunks], scratch[2 * chunks : 3 * chunks]
    z_send, z_recv, s_send, s_recv, p_send, p_recv = scratch[3 * chunks : 3 * chunks + 6]
    own_ids, by_slot, tabs, total, sums_ref, source_ref, inverse_ref = scratch[3 * chunks + 6 : 3 * chunks + 13]
    i_send, i_recv, r_send, r_recv, t_sem = scratch[3 * chunks + 13 :]
    g = lax.axis_index("grp")
    c = lax.axis_index("col")
    per_group, narrow, table_len = out_ref.shape
    chunk_rows = table_len // chunks
    sub = chunk_rows // groups

    def aligned(value, unit):
        return pl.multiple_of(value * unit, unit)

    def column_step(k, d):
        to = lax.rem(c + d, cols)
        src = table_ref.at[0, pl.ds(aligned(to, narrow), narrow), pl.ds(k * chunk_rows, chunk_rows)]
        dst = zbufs[k].at[c]
        if d == 0:
            return pltpu.make_async_copy(src, dst, z_recv.at[k, d])
        return pltpu.make_async_remote_copy(
            src, dst, z_send.at[k, d], z_recv.at[k, d], device_id=(g, to), device_id_type=MESH
        )

    def spread_step(k, d):
        to = lax.rem(g + d, groups)
        src = zbufs[k].at[:, :, pl.ds(aligned(to, sub), sub)]
        dst = spreads[k].at[pl.ds(g * cols, cols)]
        if d == 0:
            return pltpu.make_async_copy(src, dst, s_recv.at[k, d])
        return pltpu.make_async_remote_copy(
            src, dst, s_send.at[k, d], s_recv.at[k, d], device_id=(to, c), device_id_type=MESH
        )

    def group_step(k, d):
        to = lax.rem(g + d, groups)
        src = picks[k].at[pl.ds(to * per_group, per_group)]
        dst = out_ref.at[:, :, pl.ds(aligned(k * groups + g, sub), sub)]
        if d == 0:
            return pltpu.make_async_copy(src, dst, p_recv.at[k, d])
        return pltpu.make_async_remote_copy(
            src, dst, p_send.at[k, d], p_recv.at[k, d], device_id=(to, c), device_id_type=MESH
        )

    devices = groups * cols
    me = g * cols + c
    samples, tables, bag = ids_ref.shape

    def ids_step(d):
        to = lax.rem(me + d, devices)
        src, dst = by_slot.at[to], own_ids.at[me]
        if isinstance(d, int):
            return pltpu.make_async_copy(src, dst, i_recv.at[d])
        return pltpu.make_async_remote_copy(
            src, dst, i_send.at[d], i_recv.at[d],
            device_id=(to // cols, lax.rem(to, cols)), device_id_type=MESH,
        )

    def sums_step(d):
        to = lax.rem(me + d, devices)
        src, dst = total.at[to], sums_ref.at[me]
        if isinstance(d, int):
            return pltpu.make_async_copy(src, dst, r_recv.at[d])
        return pltpu.make_async_remote_copy(
            src, dst, r_send.at[d], r_recv.at[d],
            device_id=(to // cols, lax.rem(to, cols)), device_id_type=MESH,
        )

    def each_peer(act):
        def step(d, carry):
            act(d)
            return carry

        lax.fori_loop(1, devices, step, 0)

    def fetch(k):
        return pltpu.make_async_copy(
            table_ref.at[0, :, pl.ds(k * chunk_rows, chunk_rows)], tabs.at[k % 2], t_sem.at[k % 2]
        )

    tile = 512 if chunk_rows % 512 == 0 else 128
    fold = 8 if devices % 8 == 0 else 1

    def pool(k):
        fetch(k).wait()
        if k + 1 < chunks:
            fetch(k + 1).start()
        columns = chunk_rows // tile

        def piece(step, carry):
            block, part = step // columns, lax.rem(step, columns)
            rows = samples * fold
            wanted = own_ids[pl.ds(block * fold, fold)].reshape(rows, bag)
            row = lax.broadcasted_iota(jnp.int32, (rows, tile), 1) + (k * chunk_rows + part * tile)
            counts = jnp.zeros((rows, tile), jnp.float32)
            for i in range(bag):
                counts = jnp.where(wanted[:, i : i + 1] == row, counts + 1.0, counts)
            values = tabs[k % 2, :, pl.ds(aligned(part, tile), tile)]
            sums = lax.dot_general(
                counts.astype(values.dtype), values, (((1,), (1,)), ((), ())),
                preferred_element_type=jnp.float32,
            )
            where = pl.ds(block * fold, fold)
            total[where] = total[where] + sums.reshape(fold, samples, values.shape[0])
            return carry

        lax.fori_loop(0, devices // fold * columns, piece, 0)

    def finish(copy, d):
        if d == 0:
            copy.wait()
        else:
            copy.wait_recv()

    col_order = [d for d in (2, 1, 3) if d < cols] + list(range(4, cols)) + [0]
    grp_order = [d for d in ORDER if d < groups] + list(range(8, groups)) + [0]

    def order_ids(s, carry):
        by_slot[s] = ids_ref[:, pl.ds(old_ref[s], 1), :].reshape(samples, bag)
        return carry

    def locate(j, carry):
        wanted = new_ref[j]

        def look(s, found):
            held = old_ref[s]
            return jnp.where(held == wanted, s, found[0]), jnp.where(held == j, s, found[1])

        source_ref[j], inverse_ref[j] = lax.fori_loop(0, tables, look, (0, 0))
        return carry

    for k in range(min(WINDOW, chunks)):
        for d in col_order:
            column_step(k, d).start()
    fetch(0).start()
    lax.fori_loop(0, tables, order_ids, 0)
    lax.fori_loop(0, tables, locate, 0)
    each_peer(lambda d: ids_step(d).start())
    ids_step(0).start()
    total[...] = jnp.zeros_like(total)
    each_peer(lambda d: ids_step(d).wait_recv())
    ids_step(0).wait()

    def route(k):
        for d in grp_order:
            finish(spread_step(k, d), d)

        def pick(i, carry):
            picks[k][i] = spreads[k][source_ref[i]]
            return carry

        lax.fori_loop(0, groups * per_group, pick, 0)
        for d in grp_order:
            group_step(k, d).start()

    for k in range(chunks):
        for d in col_order:
            finish(column_step(k, d), d)
        for d in grp_order:
            spread_step(k, d).start()
        if k + WINDOW < chunks:
            for d in col_order:
                column_step(k + WINDOW, d).start()
        if k > 0:
            route(k - 1)
        pool(k)
    route(chunks - 1)
    each_peer(lambda d: sums_step(d).start())
    sums_step(0).start()
    for k in range(chunks):
        for d in grp_order:
            finish(group_step(k, d), d)
        for d in col_order:
            if d > 0:
                column_step(k, d).wait_send()
        for d in grp_order:
            if d > 0:
                spread_step(k, d).wait_send()
                group_step(k, d).wait_send()
    each_peer(lambda d: ids_step(d).wait_send())
    each_peer(lambda d: sums_step(d).wait())
    sums_step(0).wait()
    for t in range(tables):
        pooled_ref[:, t, :] = sums_ref[inverse_ref[t]]


def move_whole(old_tables, old_plan, new_plan, marked, groups, cols):
    _, width, table_len = old_tables.shape
    narrow = width // cols
    tables = old_plan.shape[0]
    per_group = tables // groups
    chunks = min(CHUNKS, table_len // (groups * 128))
    chunk_rows = table_len // chunks
    sub = chunk_rows // groups
    dtype = old_tables.dtype
    devices = groups * cols
    samples, _, bag = marked.shape
    sems = [
        pltpu.SemaphoreType.DMA((chunks, n)) for n in (cols, cols, groups, groups, groups, groups)
    ]
    return pl.pallas_call(
        functools.partial(whole_kernel, groups, cols, chunks),
        out_shape=(
            jax.ShapeDtypeStruct((per_group, narrow, table_len), dtype),
            jax.ShapeDtypeStruct((samples, tables, width), jnp.float32),
        ),
        in_specs=[
            pl.BlockSpec(memory_space=pltpu.SMEM),
            pl.BlockSpec(memory_space=pltpu.SMEM),
            pl.BlockSpec(memory_space=pl.ANY),
            pl.BlockSpec(memory_space=pltpu.VMEM),
        ],
        out_specs=(pl.BlockSpec(memory_space=pl.ANY), pl.BlockSpec(memory_space=pltpu.VMEM)),
        scratch_shapes=[pltpu.VMEM((cols, narrow, chunk_rows), dtype)] * chunks
        + [pltpu.VMEM((groups * cols, narrow, sub), dtype)] * chunks
        + [pltpu.VMEM((tables, narrow, sub), dtype)] * chunks
        + sems
        + [
            pltpu.VMEM((devices, samples, bag), marked.dtype),
            pltpu.VMEM((devices, samples, bag), marked.dtype),
            pltpu.VMEM((2, width, chunk_rows), dtype),
            pltpu.VMEM((devices, samples, width), jnp.float32),
            pltpu.VMEM((devices, samples, width), jnp.float32),
            pltpu.SMEM((tables,), jnp.int32),
            pltpu.SMEM((tables,), jnp.int32),
        ]
        + [pltpu.SemaphoreType.DMA((devices,))] * 4
        + [pltpu.SemaphoreType.DMA((2,))],
        compiler_params=pltpu.CompilerParams(
            has_side_effects=True, vmem_limit_bytes=48 * 1024 * 1024
        ),
    )(old_plan, new_plan, old_tables, marked)


def place_kernel(per_group, units, plan_ref, rows_ref, moved_ref, out_ref, zeros, held, in_sem, out_sem):
    own = lax.axis_index("grp") * per_group
    zeros[...] = jnp.zeros_like(zeros)

    def used(i):
        return lax.rem(i, units) * UNIT < rows_ref[plan_ref[own + i // units]]

    def window(ref, i):
        return ref.at[i // units, :, pl.ds(pl.multiple_of(lax.rem(i, units) * UNIT, UNIT), UNIT)]

    def load(i):
        return pltpu.make_async_copy(window(moved_ref, i), held.at[i], in_sem.at[i])

    def store(i, source):
        return pltpu.make_async_copy(source, window(out_ref, i), out_sem.at[i])

    def first(i, carry):
        @pl.when(used(i))
        def _():
            load(i).start()

        @pl.when(jnp.logical_not(used(i)))
        def _():
            store(i, zeros).start()

        return carry

    def second(i, carry):
        @pl.when(used(i))
        def _():
            load(i).wait()
            store(i, held.at[i]).start()

        return carry

    def third(i, carry):
        store(i, zeros).wait()
        return carry

    for step in (first, second, third):
        lax.fori_loop(0, per_group * units, step, 0)


def clear_unused(moved, new_plan, table_rows):
    per_group, narrow, table_len = moved.shape
    units = table_len // UNIT
    dma = pltpu.SemaphoreType.DMA((per_group * units,))
    return pl.pallas_call(
        functools.partial(place_kernel, per_group, units),
        out_shape=jax.ShapeDtypeStruct(moved.shape, moved.dtype),
        in_specs=[
            pl.BlockSpec(memory_space=pltpu.SMEM),
            pl.BlockSpec(memory_space=pltpu.SMEM),
            pl.BlockSpec(memory_space=pl.ANY),
        ],
        out_specs=pl.BlockSpec(memory_space=pl.ANY),
        scratch_shapes=[
            pltpu.VMEM((narrow, UNIT), moved.dtype),
            pltpu.VMEM((per_group * units, narrow, UNIT), moved.dtype),
            dma, dma,
        ],
    )(new_plan, table_rows, moved)


def vmem_bytes(chunks, units, cols, chips, caps):
    slots, room = caps
    tiles = sum(2 * chunk[1] * units * cols + cols * slots + chips * room for chunk in chunks)
    tiles += 2 * (2 * chunks[0][1] * units * cols + cols * slots + chips * room) + 3 * 1024
    return tiles * NARROW * LANES * 2


def body(old_tables, table_rows, old_plan, new_plan, ids, bag_len):
    groups = lax.axis_size("grp")
    cols = lax.axis_size("col")
    tables = old_plan.shape[0]
    per_group = tables // groups
    _, width, table_len = old_tables.shape
    units = table_len // UNIT
    chips = groups // 2
    bag_iota = lax.broadcasted_iota(jnp.int32, (1, 1, ids.shape[2]), 2)
    marked = jnp.where(bag_iota < bag_len[:, :, None], ids, -1)
    chunks = chunk_list(UNIT, width // cols // NARROW)

    over = chunks[0][1]
    slot = jnp.arange(tables, dtype=jnp.int32)
    plane, group = slot % cols, slot // cols
    part, base = (group // 2) % over, group // 2 // over
    order = group % 2 * over + part
    held = jnp.sum(jnp.where(old_plan[:, None] == slot[None, :], table_rows[None, :], 0), axis=1) // UNIT
    position = jnp.sum(jnp.where(old_plan[:, None] == new_plan[None, :], slot[None, :], 0), axis=1)
    target = position // per_group // 2
    same = base[:, None] == base[None, :]
    same_plane = plane[:, None] == plane[None, :]
    first = order[None, :] < order[:, None]
    z_off = jnp.sum(jnp.where(same & same_plane & first, held[None, :], 0), axis=1)
    ahead = (plane[None, :] < plane[:, None]) | (same_plane & first)
    c_off = jnp.sum(jnp.where(same & (target[:, None] == target[None, :]) & ahead, held[None, :], 0), axis=1)
    need = jnp.maximum(jnp.max(z_off + held), jnp.max(c_off + held))

    g = lax.axis_index("grp")
    c = lax.axis_index("col")
    chip = g // 2

    def variant(caps):
        slots, room = caps

        def run(old_tables, old_plan, new_plan, marked):
            mine = base == chip // over
            n = jnp.arange(slots, dtype=jnp.int32)[:, None]
            inside = (mine & (plane == c))[None, :] & (n >= z_off[None, :]) & (n < (z_off + held)[None, :])
            z_pick = jnp.sum(jnp.where(inside, (order * units - z_off)[None, :] + n, 0), axis=1)
            m = jnp.arange(chips * room, dtype=jnp.int32)[:, None]
            to, m = (chip + m // room) % chips, m % room
            inside = mine[None, :] & (target[None, :] == to) & (m >= c_off[None, :]) & (m < (c_off + held)[None, :])
            c_pick = jnp.sum(jnp.where(inside, (plane * slots + z_off - c_off)[None, :] + m, 0), axis=1)
            f = jnp.arange(2 * per_group * units, dtype=jnp.int32)[:, None]
            where, e = chip * 2 * per_group + f // units, f % units
            inside = (position[None, :] == where) & (e < held[None, :])
            f_pick = jnp.sum(jnp.where(inside, (base * over * room + c_off)[None, :] + e, 0), axis=1)
            picks = jnp.concatenate([z_pick, c_pick, f_pick])
            return move_tables(old_tables, old_plan, new_plan, marked, picks, groups, cols, chunks, caps)

        return run

    full = 2 * over * units
    room_full = 2 * per_group * units
    caps = [(full * s // 16, room_full * s // 16) for s in SHARES]
    caps = [cap for cap in caps if vmem_bytes(chunks, units, cols, chips, cap) < VMEM_ROOM]
    branches = [variant(cap) for cap in caps]
    if not caps or caps[-1][0] < full:

        def fallback(old_tables, old_plan, new_plan, marked):
            return move_whole(old_tables, old_plan, new_plan, marked, groups, cols)

        branches.append(fallback)
    level = sum((need > cap[0]).astype(jnp.int32) for cap in caps[: len(branches) - 1])
    moved, pooled = lax.switch(level, branches, old_tables, old_plan, new_plan, marked)
    return (clear_unused(moved, new_plan, table_rows), pooled)


def solution(mesh):
    return jax.shard_map(
        body,
        mesh=mesh,
        in_specs=(
            P(("grp", "col"), None, None),
            P(),
            P(),
            P(),
            P(("grp", "col"), None, None),
            P(("grp", "col"), None),
        ),
        out_specs=(P("grp", "col", None), P(("grp", "col"), None, None)),
        check_vma=False,
    )
```

```python
import functools

import jax
import jax.numpy as jnp
from jax import lax
from jax.experimental import pallas as pl
from jax.experimental.pallas import tpu as pltpu
from jax.sharding import PartitionSpec as P

UNIT = 4096
LANES = 128
KEYS = 256
NARROW = 16
MESH = pl.DeviceIdType.MESH
AHEAD = 3
WINDOW = 2
CHUNKS = 32
ORDER = (4, 2, 6, 3, 5, 7, 1)
VMEM_ROOM = 56 * 1024 * 1024
LAG = 2
SHARES = ((42, 38), (44, 42), (46, 46), (48, 50), (50, 54), (54, 60), (64, 64))


def chunk_list(unit, halves):
    chunks = []
    for start in range(0, unit, 8 * LANES):
        for half in range(halves):
            chunks.append((1, 4, half, start))
    return chunks


def move_kernel(shape, chunks, caps, old_ref, new_ref, table_ref, ids_ref, pick_ref, out_ref, pooled_ref, *scratch):
    groups, cols, units, width, per_group = shape
    count = len(chunks)
    spread, planes, gathered = scratch[:count], scratch[count : 2 * count], scratch[2 * count : 3 * count]
    (abuf, zbuf, cbuf, fbuf, a_send, a_recv, z_send, z_recv, c_send, c_recv, f_send, f_recv,
     own_ids, by_slot, held_ref, total, sums_ref, high_ref, low_ref, count_ref,
     i_send, i_recv, r_send, r_recv, t_sem) = scratch[3 * count :]
    g = lax.axis_index("grp")
    c = lax.axis_index("col")
    chip, core = g // 2, lax.rem(g, 2)
    chips = groups // 2
    cw = spread[0].shape[2]
    devices = groups * cols
    me = g * cols + c
    samples, tables, bag = ids_ref.shape
    slots, room = caps

    def aligned(value, unit):
        return pl.multiple_of(value * unit, unit)

    def place(k):
        stride, over, half, start = chunks[k]
        return stride, over, half, start, lax.rem(chip // stride, over)

    def spread_to(k, d):
        stride, over, half, start, mine = place(k)
        to_core = lax.rem(core + d // over, 2)
        to_part = lax.rem(mine + d % over, over)
        return to_core, to_part, (chip + (to_part - mine) * stride) * 2 + to_core

    def spread_step(k, d):
        stride, over, half, start, mine = place(k)
        slot = core * over + mine
        return pltpu.make_async_remote_copy(
            abuf.at[k % AHEAD, d], spread[k].at[pl.ds(slot * units, units)], a_send.at[k, d], a_recv.at[k, d],
            device_id=(spread_to(k, d)[2], c), device_id_type=MESH,
        )

    def spread_pack(k, d):
        stride, over, half, start, mine = place(k)
        slot = core * over + mine
        to_core, to_part, to = spread_to(k, d)
        block = start // LANES + to_core * over + to_part

        def step(e, carry):
            rows = pl.ds(aligned(e * (UNIT // LANES) + block, LANES), LANES)
            if d == 0:
                spread[k][slot * units + e] = held_ref[:, half, :, rows]
            else:
                abuf[k % AHEAD, d, e] = held_ref[:, half, :, rows]
            return carry

        lax.fori_loop(0, units, step, 0, unroll=2)

    def spread_first():
        stride, over, half, start, mine = place(0)
        slot = core * over + mine
        for d in list(range(1, 2 * over)) + [0]:
            to_core, to_part, to = spread_to(0, d)
            block = start // LANES + to_core * over + to_part

            def step(e, carry):
                src = table_ref.at[:, half, :, pl.ds(aligned(e * (UNIT // LANES) + block, LANES), LANES)]
                dst = spread[0].at[slot * units + e]
                if d == 0:
                    pltpu.make_async_copy(src, dst, a_recv.at[0, 0]).start()
                else:
                    pltpu.make_async_remote_copy(
                        src, dst, a_send.at[0, d], a_recv.at[0, d], device_id=(to, c), device_id_type=MESH
                    ).start()
                return carry

            lax.fori_loop(0, units, step, 0)

    def spread_start(k):
        others = range(1, 2 * chunks[k][1])
        if k >= AHEAD:
            for d in others:
                spread_step(k - AHEAD, d).wait_send()
        for d in others:
            spread_pack(k, d)
            spread_step(k, d).start()
        spread_pack(k, 0)

    def column_step(k, d):
        to = lax.rem(c + d, cols)
        return pltpu.make_async_remote_copy(
            zbuf.at[k % 2, to], planes[k].at[pl.ds(c * slots, slots)], z_send.at[k, d], z_recv.at[k, d],
            device_id=(g, to), device_id_type=MESH,
        )

    def chip_step(k, d):
        to = lax.rem(chip + d, chips)
        return pltpu.make_async_remote_copy(
            cbuf.at[k % 2, d], gathered[k].at[pl.ds(chip * room, room)], c_send.at[k, d], c_recv.at[k, d],
            device_id=(to * 2 + core, c), device_id_type=MESH,
        )

    def out_start(k):
        stride, over, half, start, mine = place(k)
        rows = over * LANES
        for d in (1, 0):

            def step(e, carry):
                src = fbuf.at[k % 2, d, e]
                dst = out_ref.at[
                    :, pl.ds(half * cw, cw),
                    pl.ds(aligned(e * (UNIT // LANES) + start // LANES + core * over, LANES), rows),
                ]
                if d == 0:
                    pltpu.make_async_copy(src, dst, f_recv.at[k, 0]).start()
                else:
                    pltpu.make_async_remote_copy(
                        src, dst, f_send.at[k], f_recv.at[k, 1],
                        device_id=(chip * 2 + lax.rem(core + 1, 2), c), device_id_type=MESH,
                    ).start()
                return carry

            lax.fori_loop(0, units, step, 0)

    def out_done(k, d):
        part = fbuf.at[k % 2, d]
        if d == 0:
            return pltpu.make_async_copy(part, part, f_recv.at[k, 0])
        return pltpu.make_async_remote_copy(
            part, part, f_send.at[k], f_recv.at[k, 1],
            device_id=(chip * 2 + lax.rem(core + 1, 2), c), device_id_type=MESH,
        )

    def ids_step(d):
        to = lax.rem(me + d, devices)
        src, dst = by_slot.at[to], own_ids.at[me]
        if isinstance(d, int):
            return pltpu.make_async_copy(src, dst, i_recv.at[d])
        return pltpu.make_async_remote_copy(
            src, dst, i_send.at[d], i_recv.at[d],
            device_id=(to // cols, lax.rem(to, cols)), device_id_type=MESH,
        )

    def sums_step(d):
        to = lax.rem(me + d, devices)
        src, dst = total.at[to], sums_ref.at[me]
        if isinstance(d, int):
            return pltpu.make_async_copy(src, dst, r_recv.at[d])
        return pltpu.make_async_remote_copy(
            src, dst, r_send.at[d], r_recv.at[d],
            device_id=(to // cols, lax.rem(to, cols)), device_id_type=MESH,
        )

    def each_peer(act):
        def step(d, carry):
            act(d)
            return carry

        lax.fori_loop(1, devices, step, 0)

    def fetch(e):
        rows = pl.ds(aligned(e, UNIT), UNIT)
        return pltpu.make_async_copy(table_ref.at[:, :, :, rows], held_ref.at[:, :, :, rows], t_sem.at[e])

    block, span = low_ref.shape[1] // bag, low_ref.shape[2]
    fold, blocks = block // samples, low_ref.shape[0]
    levels = units * UNIT // span // count

    def iota(shape, axis):
        return lax.broadcasted_iota(jnp.int32, shape, axis)

    def one_hot(same):
        return jnp.where(same, jnp.float32(1), jnp.float32(0)).astype(jnp.bfloat16)

    def digits(q, carry):
        keys = block * bag
        wanted = own_ids[pl.ds(q * fold, fold)].reshape(block, bag)
        high = lax.shift_right_arithmetic(wanted, span.bit_length() - 1).astype(jnp.float32)
        low = (wanted & (span - 1)).astype(jnp.float32)
        across = one_hot(lax.rem(iota((bag, keys), 1), bag) == iota((bag, keys), 0))
        spread_high = jnp.dot(high.astype(jnp.bfloat16), across, preferred_element_type=jnp.float32)
        own = iota((block, keys), 1) // bag == iota((block, keys), 0)
        high_ref[q] = jnp.where(own, spread_high, -1.0)
        down = one_hot(iota((keys, block), 0) // bag == iota((keys, block), 1))
        rows = jnp.dot(down, low.astype(jnp.bfloat16), preferred_element_type=jnp.float32)
        rows = jnp.where(lax.rem(iota((keys, bag), 0), bag) == iota((keys, bag), 1), rows, 0.0)
        ones = jnp.ones((bag, span), jnp.bfloat16)
        value = jnp.dot(rows.astype(jnp.bfloat16), ones, preferred_element_type=jnp.float32)
        low_ref[q] = one_hot(value == iota((keys, span), 1).astype(jnp.float32))
        return carry

    def count_rows(p):
        def one(q, carry):
            high = high_ref[q] - lax.convert_element_type(p * levels, jnp.float32)
            left = jnp.concatenate([one_hot(high == jnp.float32(h)) for h in range(levels)], axis=0)
            counts = jnp.dot(left, low_ref[q], preferred_element_type=jnp.float32)
            count_ref[:, pl.ds(aligned(q, block), block), :] = counts.astype(jnp.bfloat16).reshape(levels, block, span)
            return carry

        lax.fori_loop(0, blocks, one, 0)

    def pool(p):
        group = 4

        def one(h, carry):
            sums = None
            for i in range(group):
                level = h * group + i
                values = held_ref[:, :, :, pl.ds(aligned(p * levels + level, span), span)].reshape(width, span)
                term = lax.dot_general(
                    count_ref[level], values, (((1,), (1,)), ((), ())), preferred_element_type=jnp.float32
                )
                sums = term if sums is None else sums + term
            total[...] = total[...] + sums.reshape(devices, samples, width)
            return carry

        lax.fori_loop(0, levels // group, one, 0)

    def order_ids(s, carry):
        by_slot[s] = ids_ref[:, pl.ds(old_ref[s], 1), :].reshape(samples, bag)
        return carry

    c_base = slots
    f_base = slots + chips * room
    t_base = f_base + 2 * per_group * units

    def pack_columns(k):
        for d in range(1, 2 * chunks[k][1]):
            spread_step(k, d).wait_recv()
        if k == 0:
            part = spread[0].at[pl.ds(0, units)]
            pltpu.make_async_copy(part, part, a_recv.at[0, 0]).wait()
        if k >= 2:
            for d in range(1, cols):
                column_step(k - 2, d).wait_send()

        def one(n, carry):
            item = pick_ref[n]
            for z in range(cols):
                zbuf[k % 2, z, n] = spread[k][item, z]
            planes[k][c * slots + n] = spread[k][item, c]
            return carry

        lax.fori_loop(0, slots, one, 0)
        for d in COLUMN_ORDER(cols):
            column_step(k, d).start()

    def pack_chips(k):
        for d in range(1, cols):
            column_step(k, d).wait_recv()
        if k >= 2:
            for d in range(1, chips):
                chip_step(k - 2, d).wait_send()
        for d in list(range(1, chips)) + [0]:

            def one(m, carry):
                item = planes[k][pick_ref[c_base + d * room + m]]
                if d == 0:
                    gathered[k][chip * room + m] = item
                else:
                    cbuf[k % 2, d, m] = item
                return carry

            lax.fori_loop(0, room, one, 0, unroll=4)
            if d > 0:
                chip_step(k, d).start()

    def finish(k):
        stride, over, half, start, mine = place(k)
        for d in range(1, chips):
            chip_step(k, d).wait_recv()
        if k >= 2:
            out_done(k - 2, 0).wait()
            out_done(k - 2, 1).wait_send()
        for d in range(2):
            owner = lax.rem(core + d, 2)

            def one(e, carry):
                for j in range(per_group):
                    item = pick_ref[f_base + (owner * per_group + j) * units + e]
                    for b in range(over):
                        fbuf[k % 2, d, e, j, :, b * LANES : (b + 1) * LANES] = gathered[k][item + b * stride * room]
                return carry

            lax.fori_loop(0, units, one, 0)
        out_start(k)

    spread_first()
    for e in range(units):
        fetch(e).start()
    lax.fori_loop(0, tables, order_ids, 0)
    each_peer(lambda d: ids_step(d).start())
    ids_step(0).start()
    for e in range(units):
        fetch(e).wait()
    for k in range(1, min(AHEAD, count)):
        spread_start(k)
    total[...] = jnp.zeros_like(total)
    each_peer(lambda d: ids_step(d).wait_recv())
    ids_step(0).wait()
    lax.fori_loop(0, blocks, digits, 0)

    def at(t, k, act):
        @pl.when(t == k)
        def _():
            act()

    def step(t, carry):
        for k in range(count):

            def begin(k=k):
                pack_columns(k)
                if k + AHEAD < count:
                    spread_start(k + AHEAD)

            at(t, k, begin)

        @pl.when(t < count)
        def _():
            count_rows(t)

        for k in range(count):
            at(t, k + 1, functools.partial(pack_chips, k))

        @pl.when(t < count)
        def _():
            pool(t)

        @pl.when(t == count - 1)
        def _():
            each_peer(lambda d: sums_step(d).start())
            sums_step(0).start()

        for k in range(count - 1):
            at(t, k + LAG + 1, functools.partial(finish, k))
        return carry

    lax.fori_loop(0, count + LAG, step, 0)
    each_peer(lambda d: sums_step(d).wait())
    sums_step(0).wait()
    for t in range(tables):
        pooled_ref[:, t, :] = sums_ref[pick_ref[t_base + t]]
    each_peer(lambda d: ids_step(d).wait_send())
    for k in range(max(count - AHEAD, 0), count):
        for d in range(1, 2 * chunks[k][1]):
            spread_step(k, d).wait_send()
    for k in range(max(count - 2, 0), count):
        for d in range(1, cols):
            column_step(k, d).wait_send()
    finish(count - 1)
    for k in range(count):
        out_done(k, 1).wait_recv()
    for k in range(max(count - 2, 0), count):
        for d in range(1, chips):
            chip_step(k, d).wait_send()
        out_done(k, 0).wait()
        out_done(k, 1).wait_send()


def COLUMN_ORDER(cols):
    return [d for d in (2, 1, 3) if d < cols] + list(range(4, cols))


def move_tables(old_tables, old_plan, new_plan, marked, picks, groups, cols, chunks, caps):
    _, width, table_len = old_tables.shape
    narrow = width // cols
    halves = narrow // NARROW
    tables = old_plan.shape[0]
    per_group = tables // groups
    units = table_len // UNIT
    count = len(chunks)
    dtype = old_tables.dtype
    devices = groups * cols
    chips = groups // 2
    samples, _, bag = marked.shape
    slots, room = caps
    tile = (NARROW, LANES)
    over = max(chunk[1] for chunk in chunks)
    dma = pltpu.SemaphoreType.DMA
    view = old_tables.reshape(cols, halves, NARROW, table_len)
    return pl.pallas_call(
        functools.partial(move_kernel, (groups, cols, units, width, per_group), chunks, caps),
        out_shape=(
            jax.ShapeDtypeStruct((per_group, narrow, table_len), dtype),
            jax.ShapeDtypeStruct((samples, tables, width), jnp.float32),
        ),
        in_specs=[
            pl.BlockSpec(memory_space=pltpu.SMEM),
            pl.BlockSpec(memory_space=pltpu.SMEM),
            pl.BlockSpec(memory_space=pl.ANY),
            pl.BlockSpec(memory_space=pltpu.VMEM),
            pl.BlockSpec(memory_space=pltpu.SMEM),
        ],
        out_specs=(pl.BlockSpec(memory_space=pl.ANY), pl.BlockSpec(memory_space=pltpu.VMEM)),
        scratch_shapes=[pltpu.VMEM((2 * chunk[1] * units, cols) + tile, dtype) for chunk in chunks]
        + [pltpu.VMEM((cols * slots,) + tile, dtype)] * count
        + [pltpu.VMEM((chips * room,) + tile, dtype)] * count
        + [
            pltpu.VMEM((AHEAD, 2 * over, units, cols) + tile, dtype),
            pltpu.VMEM((2, cols, slots) + tile, dtype),
            pltpu.VMEM((2, chips, room) + tile, dtype),
            pltpu.VMEM((2, 2, units, per_group, NARROW, over * LANES), dtype),
            dma((count, 2 * over)), dma((count, 2 * over)),
            dma((count, cols)), dma((count, cols)),
            dma((count, chips)), dma((count, chips)),
            dma((count,)), dma((count, 2)),
            pltpu.VMEM((devices, samples, bag), marked.dtype),
            pltpu.VMEM((devices, samples, bag), marked.dtype),
            pltpu.VMEM((cols, halves, NARROW, table_len), dtype),
            pltpu.VMEM((devices, samples, width), jnp.float32),
            pltpu.VMEM((devices, samples, width), jnp.float32),
            pltpu.VMEM((devices * samples * bag // KEYS, KEYS // bag, KEYS), jnp.float32),
            pltpu.VMEM((devices * samples * bag // KEYS, KEYS, KEYS), jnp.bfloat16),
            pltpu.VMEM((table_len // KEYS // count, devices * samples, KEYS), jnp.bfloat16),
        ]
        + [dma((devices,))] * 4
        + [dma((units,))],
        compiler_params=pltpu.CompilerParams(
            has_side_effects=True, vmem_limit_bytes=60 * 1024 * 1024
        ),
    )(old_plan, new_plan, view, marked, picks)


def whole_kernel(groups, cols, chunks, old_ref, new_ref, table_ref, ids_ref, out_ref, pooled_ref, *scratch):
    zbufs, spreads, picks = scratch[:chunks], scratch[chunks : 2 * chunks], scratch[2 * chunks : 3 * chunks]
    z_send, z_recv, s_send, s_recv, p_send, p_recv = scratch[3 * chunks : 3 * chunks + 6]
    own_ids, by_slot, tabs, total, sums_ref, source_ref, inverse_ref = scratch[3 * chunks + 6 : 3 * chunks + 13]
    i_send, i_recv, r_send, r_recv, t_sem = scratch[3 * chunks + 13 :]
    g = lax.axis_index("grp")
    c = lax.axis_index("col")
    per_group, narrow, table_len = out_ref.shape
    chunk_rows = table_len // chunks
    sub = chunk_rows // groups

    def aligned(value, unit):
        return pl.multiple_of(value * unit, unit)

    def column_step(k, d):
        to = lax.rem(c + d, cols)
        src = table_ref.at[0, pl.ds(aligned(to, narrow), narrow), pl.ds(k * chunk_rows, chunk_rows)]
        dst = zbufs[k].at[c]
        if d == 0:
            return pltpu.make_async_copy(src, dst, z_recv.at[k, d])
        return pltpu.make_async_remote_copy(
            src, dst, z_send.at[k, d], z_recv.at[k, d], device_id=(g, to), device_id_type=MESH
        )

    def spread_step(k, d):
        to = lax.rem(g + d, groups)
        src = zbufs[k].at[:, :, pl.ds(aligned(to, sub), sub)]
        dst = spreads[k].at[pl.ds(g * cols, cols)]
        if d == 0:
            return pltpu.make_async_copy(src, dst, s_recv.at[k, d])
        return pltpu.make_async_remote_copy(
            src, dst, s_send.at[k, d], s_recv.at[k, d], device_id=(to, c), device_id_type=MESH
        )

    def group_step(k, d):
        to = lax.rem(g + d, groups)
        src = picks[k].at[pl.ds(to * per_group, per_group)]
        dst = out_ref.at[:, :, pl.ds(aligned(k * groups + g, sub), sub)]
        if d == 0:
            return pltpu.make_async_copy(src, dst, p_recv.at[k, d])
        return pltpu.make_async_remote_copy(
            src, dst, p_send.at[k, d], p_recv.at[k, d], device_id=(to, c), device_id_type=MESH
        )

    devices = groups * cols
    me = g * cols + c
    samples, tables, bag = ids_ref.shape

    def ids_step(d):
        to = lax.rem(me + d, devices)
        src, dst = by_slot.at[to], own_ids.at[me]
        if isinstance(d, int):
            return pltpu.make_async_copy(src, dst, i_recv.at[d])
        return pltpu.make_async_remote_copy(
            src, dst, i_send.at[d], i_recv.at[d],
            device_id=(to // cols, lax.rem(to, cols)), device_id_type=MESH,
        )

    def sums_step(d):
        to = lax.rem(me + d, devices)
        src, dst = total.at[to], sums_ref.at[me]
        if isinstance(d, int):
            return pltpu.make_async_copy(src, dst, r_recv.at[d])
        return pltpu.make_async_remote_copy(
            src, dst, r_send.at[d], r_recv.at[d],
            device_id=(to // cols, lax.rem(to, cols)), device_id_type=MESH,
        )

    def each_peer(act):
        def step(d, carry):
            act(d)
            return carry

        lax.fori_loop(1, devices, step, 0)

    def fetch(k):
        return pltpu.make_async_copy(
            table_ref.at[0, :, pl.ds(k * chunk_rows, chunk_rows)], tabs.at[k % 2], t_sem.at[k % 2]
        )

    tile = 512 if chunk_rows % 512 == 0 else 128
    fold = 8 if devices % 8 == 0 else 1

    def pool(k):
        fetch(k).wait()
        if k + 1 < chunks:
            fetch(k + 1).start()
        columns = chunk_rows // tile

        def piece(step, carry):
            block, part = step // columns, lax.rem(step, columns)
            rows = samples * fold
            wanted = own_ids[pl.ds(block * fold, fold)].reshape(rows, bag)
            row = lax.broadcasted_iota(jnp.int32, (rows, tile), 1) + (k * chunk_rows + part * tile)
            counts = jnp.zeros((rows, tile), jnp.float32)
            for i in range(bag):
                counts = jnp.where(wanted[:, i : i + 1] == row, counts + 1.0, counts)
            values = tabs[k % 2, :, pl.ds(aligned(part, tile), tile)]
            sums = lax.dot_general(
                counts.astype(values.dtype), values, (((1,), (1,)), ((), ())),
                preferred_element_type=jnp.float32,
            )
            where = pl.ds(block * fold, fold)
            total[where] = total[where] + sums.reshape(fold, samples, values.shape[0])
            return carry

        lax.fori_loop(0, devices // fold * columns, piece, 0)

    def finish(copy, d):
        if d == 0:
            copy.wait()
        else:
            copy.wait_recv()

    col_order = [d for d in (2, 1, 3) if d < cols] + list(range(4, cols)) + [0]
    grp_order = [d for d in ORDER if d < groups] + list(range(8, groups)) + [0]

    def order_ids(s, carry):
        by_slot[s] = ids_ref[:, pl.ds(old_ref[s], 1), :].reshape(samples, bag)
        return carry

    def locate(j, carry):
        wanted = new_ref[j]

        def look(s, found):
            held = old_ref[s]
            return jnp.where(held == wanted, s, found[0]), jnp.where(held == j, s, found[1])

        source_ref[j], inverse_ref[j] = lax.fori_loop(0, tables, look, (0, 0))
        return carry

    for k in range(min(WINDOW, chunks)):
        for d in col_order:
            column_step(k, d).start()
    fetch(0).start()
    lax.fori_loop(0, tables, order_ids, 0)
    lax.fori_loop(0, tables, locate, 0)
    each_peer(lambda d: ids_step(d).start())
    ids_step(0).start()
    total[...] = jnp.zeros_like(total)
    each_peer(lambda d: ids_step(d).wait_recv())
    ids_step(0).wait()

    def route(k):
        for d in grp_order:
            finish(spread_step(k, d), d)

        def pick(i, carry):
            picks[k][i] = spreads[k][source_ref[i]]
            return carry

        lax.fori_loop(0, groups * per_group, pick, 0)
        for d in grp_order:
            group_step(k, d).start()

    for k in range(chunks):
        for d in col_order:
            finish(column_step(k, d), d)
        for d in grp_order:
            spread_step(k, d).start()
        if k + WINDOW < chunks:
            for d in col_order:
                column_step(k + WINDOW, d).start()
        if k > 0:
            route(k - 1)
        pool(k)
    route(chunks - 1)
    each_peer(lambda d: sums_step(d).start())
    sums_step(0).start()
    for k in range(chunks):
        for d in grp_order:
            finish(group_step(k, d), d)
        for d in col_order:
            if d > 0:
                column_step(k, d).wait_send()
        for d in grp_order:
            if d > 0:
                spread_step(k, d).wait_send()
                group_step(k, d).wait_send()
    each_peer(lambda d: ids_step(d).wait_send())
    each_peer(lambda d: sums_step(d).wait())
    sums_step(0).wait()
    for t in range(tables):
        pooled_ref[:, t, :] = sums_ref[inverse_ref[t]]


def move_whole(old_tables, old_plan, new_plan, marked, groups, cols):
    _, width, table_len = old_tables.shape
    narrow = width // cols
    tables = old_plan.shape[0]
    per_group = tables // groups
    chunks = min(CHUNKS, table_len // (groups * 128))
    chunk_rows = table_len // chunks
    sub = chunk_rows // groups
    dtype = old_tables.dtype
    devices = groups * cols
    samples, _, bag = marked.shape
    sems = [
        pltpu.SemaphoreType.DMA((chunks, n)) for n in (cols, cols, groups, groups, groups, groups)
    ]
    return pl.pallas_call(
        functools.partial(whole_kernel, groups, cols, chunks),
        out_shape=(
            jax.ShapeDtypeStruct((per_group, narrow, table_len), dtype),
            jax.ShapeDtypeStruct((samples, tables, width), jnp.float32),
        ),
        in_specs=[
            pl.BlockSpec(memory_space=pltpu.SMEM),
            pl.BlockSpec(memory_space=pltpu.SMEM),
            pl.BlockSpec(memory_space=pl.ANY),
            pl.BlockSpec(memory_space=pltpu.VMEM),
        ],
        out_specs=(pl.BlockSpec(memory_space=pl.ANY), pl.BlockSpec(memory_space=pltpu.VMEM)),
        scratch_shapes=[pltpu.VMEM((cols, narrow, chunk_rows), dtype)] * chunks
        + [pltpu.VMEM((groups * cols, narrow, sub), dtype)] * chunks
        + [pltpu.VMEM((tables, narrow, sub), dtype)] * chunks
        + sems
        + [
            pltpu.VMEM((devices, samples, bag), marked.dtype),
            pltpu.VMEM((devices, samples, bag), marked.dtype),
            pltpu.VMEM((2, width, chunk_rows), dtype),
            pltpu.VMEM((devices, samples, width), jnp.float32),
            pltpu.VMEM((devices, samples, width), jnp.float32),
            pltpu.SMEM((tables,), jnp.int32),
            pltpu.SMEM((tables,), jnp.int32),
        ]
        + [pltpu.SemaphoreType.DMA((devices,))] * 4
        + [pltpu.SemaphoreType.DMA((2,))],
        compiler_params=pltpu.CompilerParams(
            has_side_effects=True, vmem_limit_bytes=48 * 1024 * 1024
        ),
    )(old_plan, new_plan, old_tables, marked)


def place_kernel(per_group, units, plan_ref, rows_ref, moved_ref, out_ref, zeros, held, in_sem, out_sem):
    own = lax.axis_index("grp") * per_group
    zeros[...] = jnp.zeros_like(zeros)

    def used(i):
        return lax.rem(i, units) * UNIT < rows_ref[plan_ref[own + i // units]]

    def window(ref, i):
        return ref.at[i // units, :, pl.ds(pl.multiple_of(lax.rem(i, units) * UNIT, UNIT), UNIT)]

    def load(i):
        return pltpu.make_async_copy(window(moved_ref, i), held.at[i], in_sem.at[i])

    def store(i, source):
        return pltpu.make_async_copy(source, window(out_ref, i), out_sem.at[i])

    def first(i, carry):
        @pl.when(used(i))
        def _():
            load(i).start()

        @pl.when(jnp.logical_not(used(i)))
        def _():
            store(i, zeros).start()

        return carry

    def second(i, carry):
        @pl.when(used(i))
        def _():
            load(i).wait()
            store(i, held.at[i]).start()

        return carry

    def third(i, carry):
        store(i, zeros).wait()
        return carry

    for step in (first, second, third):
        lax.fori_loop(0, per_group * units, step, 0)


def clear_unused(moved, new_plan, table_rows):
    per_group, narrow, table_len = moved.shape
    units = table_len // UNIT
    dma = pltpu.SemaphoreType.DMA((per_group * units,))
    return pl.pallas_call(
        functools.partial(place_kernel, per_group, units),
        out_shape=jax.ShapeDtypeStruct(moved.shape, moved.dtype),
        in_specs=[
            pl.BlockSpec(memory_space=pltpu.SMEM),
            pl.BlockSpec(memory_space=pltpu.SMEM),
            pl.BlockSpec(memory_space=pl.ANY),
        ],
        out_specs=pl.BlockSpec(memory_space=pl.ANY),
        scratch_shapes=[
            pltpu.VMEM((narrow, UNIT), moved.dtype),
            pltpu.VMEM((per_group * units, narrow, UNIT), moved.dtype),
            dma, dma,
        ],
    )(new_plan, table_rows, moved)


def vmem_bytes(chunks, units, cols, chips, samples, bag, caps):
    slots, room = caps
    tiles = sum(2 * chunk[1] * units * cols + cols * slots + chips * room for chunk in chunks)
    tiles += 2 * (AHEAD * chunks[0][1] * units * cols + cols * slots + chips * room) + 3 * 1024
    counts = KEYS * (samples * bag + units * UNIT // KEYS // len(chunks) * samples)
    return (tiles * NARROW * LANES + counts) * 2


def body(old_tables, table_rows, old_plan, new_plan, ids, bag_len):
    groups = lax.axis_size("grp")
    cols = lax.axis_size("col")
    tables = old_plan.shape[0]
    per_group = tables // groups
    _, width, table_len = old_tables.shape
    units = table_len // UNIT
    chips = groups // 2
    bag_iota = lax.broadcasted_iota(jnp.int32, (1, 1, ids.shape[2]), 2)
    marked = jnp.where(bag_iota < bag_len[:, :, None], ids, -1)
    chunks = chunk_list(UNIT, width // cols // NARROW)

    over = chunks[0][1]
    slot = jnp.arange(tables, dtype=jnp.int32)
    plane, group = slot % cols, slot // cols
    part, base = (group // 2) % over, group // 2 // over
    order = group % 2 * over + part
    held = jnp.sum(jnp.where(old_plan[:, None] == slot[None, :], table_rows[None, :], 0), axis=1) // UNIT
    position = jnp.sum(jnp.where(old_plan[:, None] == new_plan[None, :], slot[None, :], 0), axis=1)
    target = position // per_group // 2
    slot_of = jnp.sum(jnp.where(old_plan[None, :] == slot[:, None], slot[None, :], 0), axis=1)
    same = base[:, None] == base[None, :]
    same_plane = plane[:, None] == plane[None, :]
    first = order[None, :] < order[:, None]
    z_off = jnp.sum(jnp.where(same & same_plane & first, held[None, :], 0), axis=1)
    ahead = (plane[None, :] < plane[:, None]) | (same_plane & first)
    c_off = jnp.sum(jnp.where(same & (target[:, None] == target[None, :]) & ahead, held[None, :], 0), axis=1)
    z_need, c_need = z_off + held, c_off + held

    g = lax.axis_index("grp")
    c = lax.axis_index("col")
    chip = g // 2

    def variant(caps):
        slots, room = caps

        def run(old_tables, old_plan, new_plan, marked):
            mine = base == chip // over
            n = jnp.arange(slots, dtype=jnp.int32)[:, None]
            inside = (mine & (plane == c))[None, :] & (n >= z_off[None, :]) & (n < (z_off + held)[None, :])
            z_pick = jnp.sum(jnp.where(inside, (order * units - z_off)[None, :] + n, 0), axis=1)
            m = jnp.arange(chips * room, dtype=jnp.int32)[:, None]
            to, m = (chip + m // room) % chips, m % room
            inside = mine[None, :] & (target[None, :] == to) & (m >= c_off[None, :]) & (m < (c_off + held)[None, :])
            c_pick = jnp.sum(jnp.where(inside, (plane * slots + z_off - c_off)[None, :] + m, 0), axis=1)
            f = jnp.arange(2 * per_group * units, dtype=jnp.int32)[:, None]
            where, e = chip * 2 * per_group + f // units, f % units
            inside = (position[None, :] == where) & (e < held[None, :])
            f_pick = jnp.sum(jnp.where(inside, (base * over * room + c_off)[None, :] + e, 0), axis=1)
            picks = jnp.concatenate([z_pick, c_pick, f_pick, slot_of])
            return move_tables(old_tables, old_plan, new_plan, marked, picks, groups, cols, chunks, caps)

        return run

    full = 2 * over * units
    room_full = 2 * per_group * units
    caps = [(full * a // 64, room_full * b // 64) for a, b in SHARES]
    caps = [cap for cap in caps if vmem_bytes(chunks, units, cols, chips, ids.shape[0] * groups * cols, ids.shape[2], cap) < VMEM_ROOM]
    branches = [variant(cap) for cap in caps]
    if not caps or caps[-1][0] < full:

        def fallback(old_tables, old_plan, new_plan, marked):
            return move_whole(old_tables, old_plan, new_plan, marked, groups, cols)

        branches.append(fallback)
    misfits = (((z_need > cap[0]) | (c_need > cap[1])).astype(jnp.int32) for cap in caps[: len(branches) - 1])
    level = jnp.max(sum(misfits, start=jnp.zeros_like(z_need)))
    moved, pooled = lax.switch(level, branches, old_tables, old_plan, new_plan, marked)
    return (clear_unused(moved, new_plan, table_rows), pooled)


def solution(mesh):
    return jax.shard_map(
        body,
        mesh=mesh,
        in_specs=(
            P(("grp", "col"), None, None),
            P(),
            P(),
            P(),
            P(("grp", "col"), None, None),
            P(("grp", "col"), None),
        ),
        out_specs=(P("grp", "col", None), P(("grp", "col"), None, None)),
        check_vma=False,
    )
```

```python
import functools

import jax
import jax.numpy as jnp
from jax import lax
from jax.experimental import pallas as pl
from jax.experimental.pallas import tpu as pltpu
from jax.sharding import PartitionSpec as P

UNIT = 4096
LANES = 128
KEYS = 256
NARROW = 16
MESH = pl.DeviceIdType.MESH
AHEAD = 3
WINDOW = 2
CHUNKS = 32
ORDER = (4, 2, 6, 3, 5, 7, 1)
VMEM_ROOM = 56 * 1024 * 1024
LAG = 2
SHARES = ((42, 38), (44, 42), (46, 46), (48, 50), (50, 54), (54, 60), (64, 64))


def chunk_list(unit, halves):
    chunks = []
    for start in range(0, unit, 8 * LANES):
        for half in range(halves):
            chunks.append((1, 4, half, start))
    return chunks


def move_kernel(shape, chunks, caps, old_ref, new_ref, table_ref, ids_ref, pick_ref, out_ref, pooled_ref, *scratch):
    groups, cols, units, width, per_group = shape
    count = len(chunks)
    spread, planes, gathered = scratch[:count], scratch[count : 2 * count], scratch[2 * count : 3 * count]
    (abuf, zbuf, cbuf, fbuf, a_send, a_recv, z_send, z_recv, c_send, c_recv, f_send, f_recv,
     own_ids, by_slot, held_ref, total, sums_ref, high_ref, low_ref, count_ref,
     i_send, i_recv, r_send, r_recv, t_sem) = scratch[3 * count :]
    g = lax.axis_index("grp")
    c = lax.axis_index("col")
    chip, core = g // 2, lax.rem(g, 2)
    chips = groups // 2
    cw = spread[0].shape[2]
    devices = groups * cols
    me = g * cols + c
    samples, tables, bag = ids_ref.shape
    slots, room = caps

    def aligned(value, unit):
        return pl.multiple_of(value * unit, unit)

    def place(k):
        stride, over, half, start = chunks[k]
        return stride, over, half, start, lax.rem(chip // stride, over)

    def spread_to(k, d):
        stride, over, half, start, mine = place(k)
        to_core = lax.rem(core + d // over, 2)
        to_part = lax.rem(mine + d % over, over)
        return to_core, to_part, (chip + (to_part - mine) * stride) * 2 + to_core

    def spread_step(k, d):
        stride, over, half, start, mine = place(k)
        slot = core * over + mine
        return pltpu.make_async_remote_copy(
            abuf.at[k % AHEAD, d], spread[k].at[pl.ds(slot * units, units)], a_send.at[k, d], a_recv.at[k, d],
            device_id=(spread_to(k, d)[2], c), device_id_type=MESH,
        )

    def spread_pack(k, d):
        stride, over, half, start, mine = place(k)
        slot = core * over + mine
        to_core, to_part, to = spread_to(k, d)
        block = start // LANES + to_core * over + to_part

        def step(e, carry):
            rows = pl.ds(aligned(e * (UNIT // LANES) + block, LANES), LANES)
            if d == 0:
                spread[k][slot * units + e] = held_ref[:, half, :, rows]
            else:
                abuf[k % AHEAD, d, e] = held_ref[:, half, :, rows]
            return carry

        lax.fori_loop(0, units, step, 0, unroll=2)

    def greet(barrier):
        def signal(d, carry):
            to = lax.rem(me + d, devices)
            pl.semaphore_signal(
                barrier, inc=1, device_id=(to // cols, lax.rem(to, cols)), device_id_type=MESH
            )
            return carry

        lax.fori_loop(1, devices, signal, 0)

    def spread_start(k):
        others = range(1, 2 * chunks[k][1])
        if k >= AHEAD:
            for d in others:
                spread_step(k - AHEAD, d).wait_send()
        for d in others:
            spread_pack(k, d)
            spread_step(k, d).start()
        spread_pack(k, 0)

    def column_step(k, d):
        to = lax.rem(c + d, cols)
        return pltpu.make_async_remote_copy(
            zbuf.at[k % 2, to], planes[k].at[pl.ds(c * slots, slots)], z_send.at[k, d], z_recv.at[k, d],
            device_id=(g, to), device_id_type=MESH,
        )

    def chip_step(k, d):
        to = lax.rem(chip + d, chips)
        return pltpu.make_async_remote_copy(
            cbuf.at[k % 2, d], gathered[k].at[pl.ds(chip * room, room)], c_send.at[k, d], c_recv.at[k, d],
            device_id=(to * 2 + core, c), device_id_type=MESH,
        )

    def out_start(k, d, e):
        stride, over, half, start, mine = place(k)
        src = fbuf.at[k % 2, d, e]
        dst = out_ref.at[
            :, pl.ds(half * cw, cw),
            pl.ds(aligned(e * (UNIT // LANES) + start // LANES + core * over, LANES), over * LANES),
        ]
        if d == 0:
            pltpu.make_async_copy(src, dst, f_recv.at[k, 0]).start()
        else:
            pltpu.make_async_remote_copy(
                src, dst, f_send.at[k], f_recv.at[k, 1],
                device_id=(chip * 2 + lax.rem(core + 1, 2), c), device_id_type=MESH,
            ).start()

    def out_done(k, d):
        part = fbuf.at[k % 2, d]
        if d == 0:
            return pltpu.make_async_copy(part, part, f_recv.at[k, 0])
        return pltpu.make_async_remote_copy(
            part, part, f_send.at[k], f_recv.at[k, 1],
            device_id=(chip * 2 + lax.rem(core + 1, 2), c), device_id_type=MESH,
        )

    def ids_step(d):
        to = lax.rem(me + d, devices)
        src, dst = by_slot.at[to], own_ids.at[me]
        if isinstance(d, int):
            return pltpu.make_async_copy(src, dst, i_recv.at[d])
        return pltpu.make_async_remote_copy(
            src, dst, i_send.at[d], i_recv.at[d],
            device_id=(to // cols, lax.rem(to, cols)), device_id_type=MESH,
        )

    def sums_step(d):
        to = lax.rem(me + d, devices)
        src, dst = total.at[to], sums_ref.at[me]
        if isinstance(d, int):
            return pltpu.make_async_copy(src, dst, r_recv.at[d])
        return pltpu.make_async_remote_copy(
            src, dst, r_send.at[d], r_recv.at[d],
            device_id=(to // cols, lax.rem(to, cols)), device_id_type=MESH,
        )

    def each_peer(act):
        def step(d, carry):
            act(d)
            return carry

        lax.fori_loop(1, devices, step, 0)

    def fetch(e):
        rows = pl.ds(aligned(e, UNIT), UNIT)
        return pltpu.make_async_copy(table_ref.at[:, :, :, rows], held_ref.at[:, :, :, rows], t_sem.at[e])

    block, span = low_ref.shape[1] // bag, low_ref.shape[2]
    fold, blocks = block // samples, low_ref.shape[0]
    levels = units * UNIT // span // count

    def iota(shape, axis):
        return lax.broadcasted_iota(jnp.int32, shape, axis)

    def one_hot(same):
        return jnp.where(same, jnp.float32(1), jnp.float32(0)).astype(jnp.bfloat16)

    def digits(q, carry):
        keys = block * bag
        wanted = own_ids[pl.ds(q * fold, fold)].reshape(block, bag)
        high = lax.shift_right_arithmetic(wanted, span.bit_length() - 1).astype(jnp.float32)
        low = (wanted & (span - 1)).astype(jnp.float32)
        across = one_hot(lax.rem(iota((bag, keys), 1), bag) == iota((bag, keys), 0))
        spread_high = jnp.dot(high.astype(jnp.bfloat16), across, preferred_element_type=jnp.float32)
        own = iota((block, keys), 1) // bag == iota((block, keys), 0)
        high_ref[q] = jnp.where(own, spread_high, -1.0)
        down = one_hot(iota((keys, block), 0) // bag == iota((keys, block), 1))
        rows = jnp.dot(down, low.astype(jnp.bfloat16), preferred_element_type=jnp.float32)
        rows = jnp.where(lax.rem(iota((keys, bag), 0), bag) == iota((keys, bag), 1), rows, 0.0)
        ones = jnp.ones((bag, span), jnp.bfloat16)
        value = jnp.dot(rows.astype(jnp.bfloat16), ones, preferred_element_type=jnp.float32)
        low_ref[q] = one_hot(value == iota((keys, span), 1).astype(jnp.float32))
        return carry

    def count_rows(p):
        def one(q, carry):
            high = high_ref[q] - lax.convert_element_type(p * levels, jnp.float32)
            left = jnp.concatenate([one_hot(high == jnp.float32(h)) for h in range(levels)], axis=0)
            counts = jnp.dot(left, low_ref[q], preferred_element_type=jnp.float32)
            count_ref[:, pl.ds(aligned(q, block), block), :] = counts.astype(jnp.bfloat16).reshape(levels, block, span)
            return carry

        lax.fori_loop(0, blocks, one, 0)

    def pool(p):
        group = 4

        def one(h, carry):
            sums = None
            for i in range(group):
                level = h * group + i
                values = held_ref[:, :, :, pl.ds(aligned(p * levels + level, span), span)].reshape(width, span)
                term = lax.dot_general(
                    count_ref[level], values, (((1,), (1,)), ((), ())), preferred_element_type=jnp.float32
                )
                sums = term if sums is None else sums + term
            total[...] = total[...] + sums.reshape(devices, samples, width)
            return carry

        lax.fori_loop(0, levels // group, one, 0)

    def order_ids(s, carry):
        by_slot[s] = ids_ref[:, pl.ds(old_ref[s], 1), :].reshape(samples, bag)
        return carry

    c_base = slots
    f_base = slots + chips * room
    t_base = f_base + 2 * per_group * units

    def pack_columns(k):
        for d in range(1, 2 * chunks[k][1]):
            spread_step(k, d).wait_recv()
        if k >= 2:
            for d in range(1, cols):
                column_step(k - 2, d).wait_send()

        def one(n, carry):
            item = pick_ref[n]
            for z in range(cols):
                zbuf[k % 2, z, n] = spread[k][item, z]
            planes[k][c * slots + n] = spread[k][item, c]
            return carry

        lax.fori_loop(0, slots, one, 0)
        for d in COLUMN_ORDER(cols):
            column_step(k, d).start()

    def pack_chips(k):
        for d in range(1, cols):
            column_step(k, d).wait_recv()
        if k >= 2:
            for d in range(1, chips):
                chip_step(k - 2, d).wait_send()
        for d in list(range(1, chips)) + [0]:

            def one(m, carry):
                item = planes[k][pick_ref[c_base + d * room + m]]
                if d == 0:
                    gathered[k][chip * room + m] = item
                else:
                    cbuf[k % 2, d, m] = item
                return carry

            lax.fori_loop(0, room, one, 0, unroll=4)
            if d > 0:
                chip_step(k, d).start()

    def finish(k):
        stride, over, half, start, mine = place(k)
        for d in range(1, chips):
            chip_step(k, d).wait_recv()
        if k >= 2:
            out_done(k - 2, 0).wait()
            out_done(k - 2, 1).wait_send()
        for d in (1, 0):
            owner = lax.rem(core + d, 2)

            def one(e, carry):
                for j in range(per_group):
                    item = pick_ref[f_base + (owner * per_group + j) * units + e]
                    for b in range(over):
                        fbuf[k % 2, d, e, j, :, b * LANES : (b + 1) * LANES] = gathered[k][item + b * stride * room]
                out_start(k, d, e)
                return carry

            lax.fori_loop(0, units, one, 0)

    barrier = pltpu.get_barrier_semaphore()
    greet(barrier)
    for e in range(units):
        fetch(e).start()
    lax.fori_loop(0, tables, order_ids, 0)
    for e in range(units):
        fetch(e).wait()
    for d in range(2 * chunks[0][1]):
        spread_pack(0, d)
    pl.semaphore_wait(barrier, devices - 1)
    for d in range(1, 2 * chunks[0][1]):
        spread_step(0, d).start()
    each_peer(lambda d: ids_step(d).start())
    ids_step(0).start()
    for k in range(1, min(AHEAD, count)):
        spread_start(k)
    total[...] = jnp.zeros_like(total)
    each_peer(lambda d: ids_step(d).wait_recv())
    ids_step(0).wait()
    lax.fori_loop(0, blocks, digits, 0)

    def at(t, k, act):
        @pl.when(t == k)
        def _():
            act()

    def step(t, carry):
        for k in range(count):

            def begin(k=k):
                pack_columns(k)
                if k + AHEAD < count:
                    spread_start(k + AHEAD)

            at(t, k, begin)

        @pl.when(t < count)
        def _():
            count_rows(t)

        for k in range(count):
            at(t, k + 1, functools.partial(pack_chips, k))

        @pl.when(t < count)
        def _():
            pool(t)

        @pl.when(t == count - 1)
        def _():
            each_peer(lambda d: sums_step(d).start())
            sums_step(0).start()

        for k in range(count - 1):
            at(t, k + LAG + 1, functools.partial(finish, k))
        return carry

    lax.fori_loop(0, count + LAG, step, 0)
    each_peer(lambda d: sums_step(d).wait())
    sums_step(0).wait()
    for t in range(tables):
        pooled_ref[:, t, :] = sums_ref[pick_ref[t_base + t]]
    each_peer(lambda d: ids_step(d).wait_send())
    for k in range(max(count - AHEAD, 0), count):
        for d in range(1, 2 * chunks[k][1]):
            spread_step(k, d).wait_send()
    for k in range(max(count - 2, 0), count):
        for d in range(1, cols):
            column_step(k, d).wait_send()
    finish(count - 1)
    for k in range(count):
        out_done(k, 1).wait_recv()
    for k in range(max(count - 2, 0), count):
        for d in range(1, chips):
            chip_step(k, d).wait_send()
        out_done(k, 0).wait()
        out_done(k, 1).wait_send()


def COLUMN_ORDER(cols):
    return [d for d in (2, 1, 3) if d < cols] + list(range(4, cols))


def move_tables(old_tables, old_plan, new_plan, marked, picks, groups, cols, chunks, caps, number):
    _, width, table_len = old_tables.shape
    narrow = width // cols
    halves = narrow // NARROW
    tables = old_plan.shape[0]
    per_group = tables // groups
    units = table_len // UNIT
    count = len(chunks)
    dtype = old_tables.dtype
    devices = groups * cols
    chips = groups // 2
    samples, _, bag = marked.shape
    slots, room = caps
    tile = (NARROW, LANES)
    over = max(chunk[1] for chunk in chunks)
    dma = pltpu.SemaphoreType.DMA
    view = old_tables.reshape(cols, halves, NARROW, table_len)
    return pl.pallas_call(
        functools.partial(move_kernel, (groups, cols, units, width, per_group), chunks, caps),
        out_shape=(
            pltpu.VMEM((per_group, narrow, table_len), dtype),
            jax.ShapeDtypeStruct((samples, tables, width), jnp.float32),
        ),
        in_specs=[
            pl.BlockSpec(memory_space=pltpu.SMEM),
            pl.BlockSpec(memory_space=pltpu.SMEM),
            pl.BlockSpec(memory_space=pl.ANY),
            pl.BlockSpec(memory_space=pltpu.VMEM),
            pl.BlockSpec(memory_space=pltpu.SMEM),
        ],
        out_specs=(pl.BlockSpec(memory_space=pltpu.VMEM), pl.BlockSpec(memory_space=pltpu.VMEM)),
        scratch_shapes=[pltpu.VMEM((2 * chunk[1] * units, cols) + tile, dtype) for chunk in chunks]
        + [pltpu.VMEM((cols * slots,) + tile, dtype)] * count
        + [pltpu.VMEM((chips * room,) + tile, dtype)] * count
        + [
            pltpu.VMEM((AHEAD, 2 * over, units, cols) + tile, dtype),
            pltpu.VMEM((2, cols, slots) + tile, dtype),
            pltpu.VMEM((2, chips, room) + tile, dtype),
            pltpu.VMEM((2, 2, units, per_group, NARROW, over * LANES), dtype),
            dma((count, 2 * over)), dma((count, 2 * over)),
            dma((count, cols)), dma((count, cols)),
            dma((count, chips)), dma((count, chips)),
            dma((count,)), dma((count, 2)),
            pltpu.VMEM((devices, samples, bag), marked.dtype),
            pltpu.VMEM((devices, samples, bag), marked.dtype),
            pltpu.VMEM((cols, halves, NARROW, table_len), dtype),
            pltpu.VMEM((devices, samples, width), jnp.float32),
            pltpu.VMEM((devices, samples, width), jnp.float32),
            pltpu.VMEM((devices * samples * bag // KEYS, KEYS // bag, KEYS), jnp.float32),
            pltpu.VMEM((devices * samples * bag // KEYS, KEYS, KEYS), jnp.bfloat16),
            pltpu.VMEM((table_len // KEYS // count, devices * samples, KEYS), jnp.bfloat16),
        ]
        + [dma((devices,))] * 4
        + [dma((units,))],
        compiler_params=pltpu.CompilerParams(
            has_side_effects=True, collective_id=number, vmem_limit_bytes=54 * 1024 * 1024
        ),
    )(old_plan, new_plan, view, marked, picks)


def whole_kernel(groups, cols, chunks, old_ref, new_ref, table_ref, ids_ref, out_ref, pooled_ref, *scratch):
    zbufs, spreads, picks = scratch[:chunks], scratch[chunks : 2 * chunks], scratch[2 * chunks : 3 * chunks]
    z_send, z_recv, s_send, s_recv, p_send, p_recv = scratch[3 * chunks : 3 * chunks + 6]
    own_ids, by_slot, tabs, total, sums_ref, source_ref, inverse_ref = scratch[3 * chunks + 6 : 3 * chunks + 13]
    i_send, i_recv, r_send, r_recv, t_sem = scratch[3 * chunks + 13 :]
    g = lax.axis_index("grp")
    c = lax.axis_index("col")
    per_group, narrow, table_len = out_ref.shape
    chunk_rows = table_len // chunks
    sub = chunk_rows // groups

    def aligned(value, unit):
        return pl.multiple_of(value * unit, unit)

    def column_step(k, d):
        to = lax.rem(c + d, cols)
        src = table_ref.at[0, pl.ds(aligned(to, narrow), narrow), pl.ds(k * chunk_rows, chunk_rows)]
        dst = zbufs[k].at[c]
        if d == 0:
            return pltpu.make_async_copy(src, dst, z_recv.at[k, d])
        return pltpu.make_async_remote_copy(
            src, dst, z_send.at[k, d], z_recv.at[k, d], device_id=(g, to), device_id_type=MESH
        )

    def spread_step(k, d):
        to = lax.rem(g + d, groups)
        src = zbufs[k].at[:, :, pl.ds(aligned(to, sub), sub)]
        dst = spreads[k].at[pl.ds(g * cols, cols)]
        if d == 0:
            return pltpu.make_async_copy(src, dst, s_recv.at[k, d])
        return pltpu.make_async_remote_copy(
            src, dst, s_send.at[k, d], s_recv.at[k, d], device_id=(to, c), device_id_type=MESH
        )

    def group_step(k, d):
        to = lax.rem(g + d, groups)
        src = picks[k].at[pl.ds(to * per_group, per_group)]
        dst = out_ref.at[:, :, pl.ds(aligned(k * groups + g, sub), sub)]
        if d == 0:
            return pltpu.make_async_copy(src, dst, p_recv.at[k, d])
        return pltpu.make_async_remote_copy(
            src, dst, p_send.at[k, d], p_recv.at[k, d], device_id=(to, c), device_id_type=MESH
        )

    devices = groups * cols
    me = g * cols + c
    samples, tables, bag = ids_ref.shape

    def ids_step(d):
        to = lax.rem(me + d, devices)
        src, dst = by_slot.at[to], own_ids.at[me]
        if isinstance(d, int):
            return pltpu.make_async_copy(src, dst, i_recv.at[d])
        return pltpu.make_async_remote_copy(
            src, dst, i_send.at[d], i_recv.at[d],
            device_id=(to // cols, lax.rem(to, cols)), device_id_type=MESH,
        )

    def sums_step(d):
        to = lax.rem(me + d, devices)
        src, dst = total.at[to], sums_ref.at[me]
        if isinstance(d, int):
            return pltpu.make_async_copy(src, dst, r_recv.at[d])
        return pltpu.make_async_remote_copy(
            src, dst, r_send.at[d], r_recv.at[d],
            device_id=(to // cols, lax.rem(to, cols)), device_id_type=MESH,
        )

    def each_peer(act):
        def step(d, carry):
            act(d)
            return carry

        lax.fori_loop(1, devices, step, 0)

    def fetch(k):
        return pltpu.make_async_copy(
            table_ref.at[0, :, pl.ds(k * chunk_rows, chunk_rows)], tabs.at[k % 2], t_sem.at[k % 2]
        )

    tile = 512 if chunk_rows % 512 == 0 else 128
    fold = 8 if devices % 8 == 0 else 1

    def pool(k):
        fetch(k).wait()
        if k + 1 < chunks:
            fetch(k + 1).start()
        columns = chunk_rows // tile

        def piece(step, carry):
            block, part = step // columns, lax.rem(step, columns)
            rows = samples * fold
            wanted = own_ids[pl.ds(block * fold, fold)].reshape(rows, bag)
            row = lax.broadcasted_iota(jnp.int32, (rows, tile), 1) + (k * chunk_rows + part * tile)
            counts = jnp.zeros((rows, tile), jnp.float32)
            for i in range(bag):
                counts = jnp.where(wanted[:, i : i + 1] == row, counts + 1.0, counts)
            values = tabs[k % 2, :, pl.ds(aligned(part, tile), tile)]
            sums = lax.dot_general(
                counts.astype(values.dtype), values, (((1,), (1,)), ((), ())),
                preferred_element_type=jnp.float32,
            )
            where = pl.ds(block * fold, fold)
            total[where] = total[where] + sums.reshape(fold, samples, values.shape[0])
            return carry

        lax.fori_loop(0, devices // fold * columns, piece, 0)

    def finish(copy, d):
        if d == 0:
            copy.wait()
        else:
            copy.wait_recv()

    col_order = [d for d in (2, 1, 3) if d < cols] + list(range(4, cols)) + [0]
    grp_order = [d for d in ORDER if d < groups] + list(range(8, groups)) + [0]

    def order_ids(s, carry):
        by_slot[s] = ids_ref[:, pl.ds(old_ref[s], 1), :].reshape(samples, bag)
        return carry

    def locate(j, carry):
        wanted = new_ref[j]

        def look(s, found):
            held = old_ref[s]
            return jnp.where(held == wanted, s, found[0]), jnp.where(held == j, s, found[1])

        source_ref[j], inverse_ref[j] = lax.fori_loop(0, tables, look, (0, 0))
        return carry

    for k in range(min(WINDOW, chunks)):
        for d in col_order:
            column_step(k, d).start()
    fetch(0).start()
    lax.fori_loop(0, tables, order_ids, 0)
    lax.fori_loop(0, tables, locate, 0)
    each_peer(lambda d: ids_step(d).start())
    ids_step(0).start()
    total[...] = jnp.zeros_like(total)
    each_peer(lambda d: ids_step(d).wait_recv())
    ids_step(0).wait()

    def route(k):
        for d in grp_order:
            finish(spread_step(k, d), d)

        def pick(i, carry):
            picks[k][i] = spreads[k][source_ref[i]]
            return carry

        lax.fori_loop(0, groups * per_group, pick, 0)
        for d in grp_order:
            group_step(k, d).start()

    for k in range(chunks):
        for d in col_order:
            finish(column_step(k, d), d)
        for d in grp_order:
            spread_step(k, d).start()
        if k + WINDOW < chunks:
            for d in col_order:
                column_step(k + WINDOW, d).start()
        if k > 0:
            route(k - 1)
        pool(k)
    route(chunks - 1)
    each_peer(lambda d: sums_step(d).start())
    sums_step(0).start()
    for k in range(chunks):
        for d in grp_order:
            finish(group_step(k, d), d)
        for d in col_order:
            if d > 0:
                column_step(k, d).wait_send()
        for d in grp_order:
            if d > 0:
                spread_step(k, d).wait_send()
                group_step(k, d).wait_send()
    each_peer(lambda d: ids_step(d).wait_send())
    each_peer(lambda d: sums_step(d).wait())
    sums_step(0).wait()
    for t in range(tables):
        pooled_ref[:, t, :] = sums_ref[inverse_ref[t]]


def move_whole(old_tables, old_plan, new_plan, marked, groups, cols):
    _, width, table_len = old_tables.shape
    narrow = width // cols
    tables = old_plan.shape[0]
    per_group = tables // groups
    chunks = min(CHUNKS, table_len // (groups * 128))
    chunk_rows = table_len // chunks
    sub = chunk_rows // groups
    dtype = old_tables.dtype
    devices = groups * cols
    samples, _, bag = marked.shape
    sems = [
        pltpu.SemaphoreType.DMA((chunks, n)) for n in (cols, cols, groups, groups, groups, groups)
    ]
    return pl.pallas_call(
        functools.partial(whole_kernel, groups, cols, chunks),
        out_shape=(
            jax.ShapeDtypeStruct((per_group, narrow, table_len), dtype),
            jax.ShapeDtypeStruct((samples, tables, width), jnp.float32),
        ),
        in_specs=[
            pl.BlockSpec(memory_space=pltpu.SMEM),
            pl.BlockSpec(memory_space=pltpu.SMEM),
            pl.BlockSpec(memory_space=pl.ANY),
            pl.BlockSpec(memory_space=pltpu.VMEM),
        ],
        out_specs=(pl.BlockSpec(memory_space=pl.ANY), pl.BlockSpec(memory_space=pltpu.VMEM)),
        scratch_shapes=[pltpu.VMEM((cols, narrow, chunk_rows), dtype)] * chunks
        + [pltpu.VMEM((groups * cols, narrow, sub), dtype)] * chunks
        + [pltpu.VMEM((tables, narrow, sub), dtype)] * chunks
        + sems
        + [
            pltpu.VMEM((devices, samples, bag), marked.dtype),
            pltpu.VMEM((devices, samples, bag), marked.dtype),
            pltpu.VMEM((2, width, chunk_rows), dtype),
            pltpu.VMEM((devices, samples, width), jnp.float32),
            pltpu.VMEM((devices, samples, width), jnp.float32),
            pltpu.SMEM((tables,), jnp.int32),
            pltpu.SMEM((tables,), jnp.int32),
        ]
        + [pltpu.SemaphoreType.DMA((devices,))] * 4
        + [pltpu.SemaphoreType.DMA((2,))],
        compiler_params=pltpu.CompilerParams(
            has_side_effects=True, vmem_limit_bytes=48 * 1024 * 1024
        ),
    )(old_plan, new_plan, old_tables, marked)


def place_kernel(per_group, units, plan_ref, rows_ref, moved_ref, out_ref, zeros, out_sem):
    own = lax.axis_index("grp") * per_group
    zeros[...] = jnp.zeros_like(zeros)

    def used(i):
        return lax.rem(i, units) * UNIT < rows_ref[plan_ref[own + i // units]]

    def window(ref, i):
        return ref.at[i // units, :, pl.ds(pl.multiple_of(lax.rem(i, units) * UNIT, UNIT), UNIT)]

    def store(i, source):
        return pltpu.make_async_copy(source, window(out_ref, i), out_sem.at[i])

    def first(i, carry):
        @pl.when(used(i))
        def _():
            store(i, window(moved_ref, i)).start()

        @pl.when(jnp.logical_not(used(i)))
        def _():
            store(i, zeros).start()

        return carry

    def third(i, carry):
        store(i, zeros).wait()
        return carry

    for step in (first, third):
        lax.fori_loop(0, per_group * units, step, 0)


def clear_unused(moved, new_plan, table_rows):
    per_group, narrow, table_len = moved.shape
    units = table_len // UNIT
    dma = pltpu.SemaphoreType.DMA((per_group * units,))
    return pl.pallas_call(
        functools.partial(place_kernel, per_group, units),
        out_shape=pltpu.HBM(moved.shape, moved.dtype),
        in_specs=[
            pl.BlockSpec(memory_space=pltpu.SMEM),
            pl.BlockSpec(memory_space=pltpu.SMEM),
            pl.BlockSpec(memory_space=pltpu.VMEM),
        ],
        out_specs=pl.BlockSpec(memory_space=pltpu.HBM),
        scratch_shapes=[pltpu.VMEM((narrow, UNIT), moved.dtype), dma],
        compiler_params=pltpu.CompilerParams(vmem_limit_bytes=12 * 1024 * 1024),
    )(new_plan, table_rows, moved)


def vmem_bytes(chunks, units, cols, chips, samples, bag, caps):
    slots, room = caps
    tiles = sum(2 * chunk[1] * units * cols + cols * slots + chips * room for chunk in chunks)
    tiles += 2 * (AHEAD * chunks[0][1] * units * cols + cols * slots + chips * room) + 3 * 1024
    counts = KEYS * (samples * bag + units * UNIT // KEYS // len(chunks) * samples)
    return (tiles * NARROW * LANES + counts) * 2


def body(old_tables, table_rows, old_plan, new_plan, ids, bag_len):
    groups = lax.axis_size("grp")
    cols = lax.axis_size("col")
    tables = old_plan.shape[0]
    per_group = tables // groups
    _, width, table_len = old_tables.shape
    units = table_len // UNIT
    chips = groups // 2
    bag_iota = lax.broadcasted_iota(jnp.int32, (1, 1, ids.shape[2]), 2)
    marked = jnp.where(bag_iota < bag_len[:, :, None], ids, -1)
    chunks = chunk_list(UNIT, width // cols // NARROW)

    over = chunks[0][1]
    slot = jnp.arange(tables, dtype=jnp.int32)
    plane, group = slot % cols, slot // cols
    part, base = (group // 2) % over, group // 2 // over
    order = group % 2 * over + part
    held = jnp.sum(jnp.where(old_plan[:, None] == slot[None, :], table_rows[None, :], 0), axis=1) // UNIT
    position = jnp.sum(jnp.where(old_plan[:, None] == new_plan[None, :], slot[None, :], 0), axis=1)
    target = position // per_group // 2
    slot_of = jnp.sum(jnp.where(old_plan[None, :] == slot[:, None], slot[None, :], 0), axis=1)
    same = base[:, None] == base[None, :]
    same_plane = plane[:, None] == plane[None, :]
    first = order[None, :] < order[:, None]
    z_off = jnp.sum(jnp.where(same & same_plane & first, held[None, :], 0), axis=1)
    ahead = (plane[None, :] < plane[:, None]) | (same_plane & first)
    c_off = jnp.sum(jnp.where(same & (target[:, None] == target[None, :]) & ahead, held[None, :], 0), axis=1)
    z_need, c_need = z_off + held, c_off + held

    g = lax.axis_index("grp")
    c = lax.axis_index("col")
    chip = g // 2

    def variant(number, caps):
        slots, room = caps

        def run(old_tables, table_rows, old_plan, new_plan, marked):
            mine = base == chip // over
            n = jnp.arange(slots, dtype=jnp.int32)[:, None]
            inside = (mine & (plane == c))[None, :] & (n >= z_off[None, :]) & (n < (z_off + held)[None, :])
            z_pick = jnp.sum(jnp.where(inside, (order * units - z_off)[None, :] + n, 0), axis=1)
            m = jnp.arange(chips * room, dtype=jnp.int32)[:, None]
            to, m = (chip + m // room) % chips, m % room
            inside = mine[None, :] & (target[None, :] == to) & (m >= c_off[None, :]) & (m < (c_off + held)[None, :])
            c_pick = jnp.sum(jnp.where(inside, (plane * slots + z_off - c_off)[None, :] + m, 0), axis=1)
            f = jnp.arange(2 * per_group * units, dtype=jnp.int32)[:, None]
            where, e = chip * 2 * per_group + f // units, f % units
            inside = (position[None, :] == where) & (e < held[None, :])
            f_pick = jnp.sum(jnp.where(inside, (base * over * room + c_off)[None, :] + e, 0), axis=1)
            picks = jnp.concatenate([z_pick, c_pick, f_pick, slot_of])
            moved, pooled = move_tables(
                old_tables, old_plan, new_plan, marked, picks, groups, cols, chunks, caps, number
            )
            return clear_unused(moved, new_plan, table_rows), pooled

        return run

    full = 2 * over * units
    room_full = 2 * per_group * units
    caps = [(full * a // 64, room_full * b // 64) for a, b in SHARES]
    caps = [cap for cap in caps if vmem_bytes(chunks, units, cols, chips, ids.shape[0] * groups * cols, ids.shape[2], cap) < VMEM_ROOM]
    branches = [variant(number, cap) for number, cap in enumerate(caps)]
    if not caps or caps[-1][0] < full:

        def fallback(old_tables, table_rows, old_plan, new_plan, marked):
            moved, pooled = move_whole(old_tables, old_plan, new_plan, marked, groups, cols)
            return clear_unused(moved, new_plan, table_rows), pooled

        branches.append(fallback)
    misfits = (((z_need > cap[0]) | (c_need > cap[1])).astype(jnp.int32) for cap in caps[: len(branches) - 1])
    level = jnp.max(sum(misfits, start=jnp.zeros_like(z_need)))
    return lax.switch(level, branches, old_tables, table_rows, old_plan, new_plan, marked)


def solution(mesh):
    return jax.shard_map(
        body,
        mesh=mesh,
        in_specs=(
            P(("grp", "col"), None, None),
            P(),
            P(),
            P(),
            P(("grp", "col"), None, None),
            P(("grp", "col"), None),
        ),
        out_specs=(P("grp", "col", None), P(("grp", "col"), None, None)),
        check_vma=False,
    )
```

```python
import functools

import jax
import jax.numpy as jnp
from jax import lax
from jax.experimental import pallas as pl
from jax.experimental.pallas import tpu as pltpu
from jax.sharding import PartitionSpec as P

UNIT = 4096
LANES = 128
KEYS = 256
NARROW = 16
MESH = pl.DeviceIdType.MESH
AHEAD = 3
WINDOW = 2
CHUNKS = 32
ORDER = (4, 2, 6, 3, 5, 7, 1)
VMEM_ROOM = 56 * 1024 * 1024
LAG = 2
SHARES = ((42, 38), (44, 42), (46, 46), (48, 50), (50, 54), (54, 60), (64, 64))


def chunk_list(unit, halves):
    chunks = []
    for start in range(0, unit, 8 * LANES):
        for half in range(halves):
            chunks.append((1, 4, half, start))
    return chunks


def move_kernel(shape, chunks, caps, old_ref, new_ref, table_ref, ids_ref, pick_ref, out_ref, pooled_ref, *scratch):
    groups, cols, units, width, per_group = shape
    count = len(chunks)
    spread, planes, gathered = scratch[:count], scratch[count : 2 * count], scratch[2 * count : 3 * count]
    (abuf, zbuf, cbuf, fbuf, a_send, a_recv, z_send, z_recv, c_send, c_recv, f_send, f_recv,
     own_ids, by_slot, held_ref, total, sums_ref, high_ref, low_ref, count_ref,
     i_send, i_recv, r_send, r_recv, t_sem) = scratch[3 * count :]
    g = lax.axis_index("grp")
    c = lax.axis_index("col")
    chip, core = g // 2, lax.rem(g, 2)
    chips = groups // 2
    cw = spread[0].shape[2]
    devices = groups * cols
    me = g * cols + c
    samples, tables, bag = ids_ref.shape
    slots, room = caps

    def aligned(value, unit):
        return pl.multiple_of(value * unit, unit)

    def place(k):
        stride, over, half, start = chunks[k]
        return stride, over, half, start, lax.rem(chip // stride, over)

    def spread_to(k, d):
        stride, over, half, start, mine = place(k)
        to_core = lax.rem(core + d // over, 2)
        to_part = lax.rem(mine + d % over, over)
        return to_core, to_part, (chip + (to_part - mine) * stride) * 2 + to_core

    def spread_step(k, d):
        stride, over, half, start, mine = place(k)
        slot = core * over + mine
        return pltpu.make_async_remote_copy(
            abuf.at[k % AHEAD, d], spread[k].at[pl.ds(slot * units, units)], a_send.at[k, d], a_recv.at[k, d],
            device_id=(spread_to(k, d)[2], c), device_id_type=MESH,
        )

    def spread_pack(k, d):
        stride, over, half, start, mine = place(k)
        slot = core * over + mine
        to_core, to_part, to = spread_to(k, d)
        block = start // LANES + to_core * over + to_part

        def step(e, carry):
            rows = pl.ds(aligned(e * (UNIT // LANES) + block, LANES), LANES)
            if d == 0:
                spread[k][slot * units + e] = held_ref[:, half, :, rows]
            else:
                abuf[k % AHEAD, d, e] = held_ref[:, half, :, rows]
            return carry

        lax.fori_loop(0, units, step, 0, unroll=2)

    def greet(barrier):
        def signal(d, carry):
            to = lax.rem(me + d, devices)
            pl.semaphore_signal(
                barrier, inc=1, device_id=(to // cols, lax.rem(to, cols)), device_id_type=MESH
            )
            return carry

        lax.fori_loop(1, devices, signal, 0)

    def spread_start(k):
        others = range(1, 2 * chunks[k][1])
        if k >= AHEAD:
            for d in others:
                spread_step(k - AHEAD, d).wait_send()
        for d in others:
            spread_pack(k, d)
            spread_step(k, d).start()
        spread_pack(k, 0)

    def column_step(k, d):
        to = lax.rem(c + d, cols)
        return pltpu.make_async_remote_copy(
            zbuf.at[k % 2, to], planes[k].at[pl.ds(c * slots, slots)], z_send.at[k, d], z_recv.at[k, d],
            device_id=(g, to), device_id_type=MESH,
        )

    def chip_step(k, d):
        to = lax.rem(chip + d, chips)
        return pltpu.make_async_remote_copy(
            cbuf.at[k % 2, d], gathered[k].at[pl.ds(chip * room, room)], c_send.at[k, d], c_recv.at[k, d],
            device_id=(to * 2 + core, c), device_id_type=MESH,
        )

    def out_start(k, d, e):
        stride, over, half, start, mine = place(k)
        src = fbuf.at[k % 2, d, e]
        dst = out_ref.at[
            :, pl.ds(half * cw, cw),
            pl.ds(aligned(e * (UNIT // LANES) + start // LANES + core * over, LANES), over * LANES),
        ]
        if d == 0:
            pltpu.make_async_copy(src, dst, f_recv.at[k, 0]).start()
        else:
            pltpu.make_async_remote_copy(
                src, dst, f_send.at[k], f_recv.at[k, 1],
                device_id=(chip * 2 + lax.rem(core + 1, 2), c), device_id_type=MESH,
            ).start()

    def out_done(k, d):
        part = fbuf.at[k % 2, d]
        if d == 0:
            return pltpu.make_async_copy(part, part, f_recv.at[k, 0])
        return pltpu.make_async_remote_copy(
            part, part, f_send.at[k], f_recv.at[k, 1],
            device_id=(chip * 2 + lax.rem(core + 1, 2), c), device_id_type=MESH,
        )

    def ids_step(d):
        to = lax.rem(me + d, devices)
        src, dst = by_slot.at[to], own_ids.at[me]
        if isinstance(d, int):
            return pltpu.make_async_copy(src, dst, i_recv.at[d])
        return pltpu.make_async_remote_copy(
            src, dst, i_send.at[d], i_recv.at[d],
            device_id=(to // cols, lax.rem(to, cols)), device_id_type=MESH,
        )

    def sums_step(d):
        to = lax.rem(me + d, devices)
        src, dst = total.at[to], sums_ref.at[me]
        if isinstance(d, int):
            return pltpu.make_async_copy(src, dst, r_recv.at[d])
        return pltpu.make_async_remote_copy(
            src, dst, r_send.at[d], r_recv.at[d],
            device_id=(to // cols, lax.rem(to, cols)), device_id_type=MESH,
        )

    def each_peer(act):
        def step(d, carry):
            act(d)
            return carry

        lax.fori_loop(1, devices, step, 0)

    def fetch(e):
        rows = pl.ds(aligned(e, UNIT), UNIT)
        return pltpu.make_async_copy(table_ref.at[:, :, :, rows], held_ref.at[:, :, :, rows], t_sem.at[e])

    block, span = low_ref.shape[1] // bag, low_ref.shape[2]
    fold, blocks = block // samples, low_ref.shape[0]
    levels = units * UNIT // span // count

    def iota(shape, axis):
        return lax.broadcasted_iota(jnp.int32, shape, axis)

    def one_hot(same):
        return jnp.where(same, jnp.float32(1), jnp.float32(0)).astype(jnp.bfloat16)

    def digits(q, carry):
        keys = block * bag
        wanted = own_ids[pl.ds(q * fold, fold)].reshape(block, bag)
        high = lax.shift_right_arithmetic(wanted, span.bit_length() - 1).astype(jnp.float32)
        low = (wanted & (span - 1)).astype(jnp.float32)
        across = one_hot(lax.rem(iota((bag, keys), 1), bag) == iota((bag, keys), 0))
        spread_high = jnp.dot(high.astype(jnp.bfloat16), across, preferred_element_type=jnp.float32)
        own = iota((block, keys), 1) // bag == iota((block, keys), 0)
        high_ref[q] = jnp.where(own, spread_high, -1.0)
        down = one_hot(iota((keys, block), 0) // bag == iota((keys, block), 1))
        rows = jnp.dot(down, low.astype(jnp.bfloat16), preferred_element_type=jnp.float32)
        rows = jnp.where(lax.rem(iota((keys, bag), 0), bag) == iota((keys, bag), 1), rows, 0.0)
        ones = jnp.ones((bag, span), jnp.bfloat16)
        value = jnp.dot(rows.astype(jnp.bfloat16), ones, preferred_element_type=jnp.float32)
        low_ref[q] = one_hot(value == iota((keys, span), 1).astype(jnp.float32))
        return carry

    def count_rows(p):
        def one(q, carry):
            high = high_ref[q] - lax.convert_element_type(p * levels, jnp.float32)
            left = jnp.concatenate([one_hot(high == jnp.float32(h)) for h in range(levels)], axis=0)
            counts = jnp.dot(left, low_ref[q], preferred_element_type=jnp.float32)
            count_ref[:, pl.ds(aligned(q, block), block), :] = counts.astype(jnp.bfloat16).reshape(levels, block, span)
            return carry

        lax.fori_loop(0, blocks, one, 0)

    def pool(p):
        group = 4

        def one(h, carry):
            sums = None
            for i in range(group):
                level = h * group + i
                values = held_ref[:, :, :, pl.ds(aligned(p * levels + level, span), span)].reshape(width, span)
                term = lax.dot_general(
                    count_ref[level], values, (((1,), (1,)), ((), ())), preferred_element_type=jnp.float32
                )
                sums = term if sums is None else sums + term
            total[...] = total[...] + sums.reshape(devices, samples, width)
            return carry

        lax.fori_loop(0, levels // group, one, 0)

    def order_ids(s, carry):
        by_slot[s] = ids_ref[:, pl.ds(old_ref[s], 1), :].reshape(samples, bag)
        return carry

    c_base = slots
    f_base = slots + chips * room
    t_base = f_base + 2 * per_group * units

    def pack_columns(k):
        for d in range(1, 2 * chunks[k][1]):
            spread_step(k, d).wait_recv()
        if k >= 2:
            for d in range(1, cols):
                column_step(k - 2, d).wait_send()

        def one(n, carry):
            item = pick_ref[n]
            for z in range(cols):
                zbuf[k % 2, z, n] = spread[k][item, z]
            planes[k][c * slots + n] = spread[k][item, c]
            return carry

        lax.fori_loop(0, slots, one, 0, unroll=2)
        for d in COLUMN_ORDER(cols):
            column_step(k, d).start()

    def pack_chips(k):
        for d in range(1, cols):
            column_step(k, d).wait_recv()
        if k >= 2:
            for d in range(1, chips):
                chip_step(k - 2, d).wait_send()
        for d in list(range(1, chips)) + [0]:

            def one(m, carry):
                item = planes[k][pick_ref[c_base + d * room + m]]
                if d == 0:
                    gathered[k][chip * room + m] = item
                else:
                    cbuf[k % 2, d, m] = item
                return carry

            lax.fori_loop(0, room, one, 0, unroll=4)
            if d > 0:
                chip_step(k, d).start()

    def finish(k):
        stride, over, half, start, mine = place(k)
        for d in range(1, chips):
            chip_step(k, d).wait_recv()
        if k >= 2:
            out_done(k - 2, 0).wait()
            out_done(k - 2, 1).wait_send()
        for d in (1, 0):
            owner = lax.rem(core + d, 2)

            def one(e, carry):
                for j in range(per_group):
                    item = pick_ref[f_base + (owner * per_group + j) * units + e]
                    for b in range(over):
                        fbuf[k % 2, d, e, j, :, b * LANES : (b + 1) * LANES] = gathered[k][item + b * stride * room]
                out_start(k, d, e)
                return carry

            lax.fori_loop(0, units, one, 0)

    barrier = pltpu.get_barrier_semaphore()
    greet(barrier)
    for e in range(units):
        fetch(e).start()
    lax.fori_loop(0, tables, order_ids, 0)
    for e in range(units):
        fetch(e).wait()
    for d in range(2 * chunks[0][1]):
        spread_pack(0, d)
    pl.semaphore_wait(barrier, devices - 1)
    for d in range(1, 2 * chunks[0][1]):
        spread_step(0, d).start()
    each_peer(lambda d: ids_step(d).start())
    ids_step(0).start()
    for k in range(1, min(AHEAD, count)):
        spread_start(k)
    total[...] = jnp.zeros_like(total)
    each_peer(lambda d: ids_step(d).wait_recv())
    ids_step(0).wait()
    lax.fori_loop(0, blocks, digits, 0)

    def at(t, k, act):
        @pl.when(t == k)
        def _():
            act()

    def step(t, carry):
        for k in range(count):

            def begin(k=k):
                pack_columns(k)
                if k + AHEAD < count:
                    spread_start(k + AHEAD)

            at(t, k, begin)

        @pl.when(t < count)
        def _():
            count_rows(t)

        for k in range(count):
            at(t, k + 1, functools.partial(pack_chips, k))

        @pl.when(t < count)
        def _():
            pool(t)

        @pl.when(t == count - 1)
        def _():
            each_peer(lambda d: sums_step(d).start())
            sums_step(0).start()

        for k in range(count - 1):
            at(t, k + LAG + 1, functools.partial(finish, k))
        return carry

    lax.fori_loop(0, count + LAG, step, 0)
    each_peer(lambda d: sums_step(d).wait())
    sums_step(0).wait()
    for t in range(tables):
        pooled_ref[:, t, :] = sums_ref[pick_ref[t_base + t]]
    each_peer(lambda d: ids_step(d).wait_send())
    for k in range(max(count - AHEAD, 0), count):
        for d in range(1, 2 * chunks[k][1]):
            spread_step(k, d).wait_send()
    for k in range(max(count - 2, 0), count):
        for d in range(1, cols):
            column_step(k, d).wait_send()
    finish(count - 1)
    for k in range(count):
        out_done(k, 1).wait_recv()
    for k in range(max(count - 2, 0), count):
        for d in range(1, chips):
            chip_step(k, d).wait_send()
        out_done(k, 0).wait()
        out_done(k, 1).wait_send()


def COLUMN_ORDER(cols):
    return [d for d in (2, 1, 3) if d < cols] + list(range(4, cols))


def move_tables(old_tables, old_plan, new_plan, marked, picks, groups, cols, chunks, caps, number):
    _, width, table_len = old_tables.shape
    narrow = width // cols
    halves = narrow // NARROW
    tables = old_plan.shape[0]
    per_group = tables // groups
    units = table_len // UNIT
    count = len(chunks)
    dtype = old_tables.dtype
    devices = groups * cols
    chips = groups // 2
    samples, _, bag = marked.shape
    slots, room = caps
    tile = (NARROW, LANES)
    over = max(chunk[1] for chunk in chunks)
    dma = pltpu.SemaphoreType.DMA
    view = old_tables.reshape(cols, halves, NARROW, table_len)
    return pl.pallas_call(
        functools.partial(move_kernel, (groups, cols, units, width, per_group), chunks, caps),
        out_shape=(
            pltpu.VMEM((per_group, narrow, table_len), dtype),
            jax.ShapeDtypeStruct((samples, tables, width), jnp.float32),
        ),
        in_specs=[
            pl.BlockSpec(memory_space=pltpu.SMEM),
            pl.BlockSpec(memory_space=pltpu.SMEM),
            pl.BlockSpec(memory_space=pl.ANY),
            pl.BlockSpec(memory_space=pltpu.VMEM),
            pl.BlockSpec(memory_space=pltpu.SMEM),
        ],
        out_specs=(pl.BlockSpec(memory_space=pltpu.VMEM), pl.BlockSpec(memory_space=pltpu.VMEM)),
        scratch_shapes=[pltpu.VMEM((2 * chunk[1] * units, cols) + tile, dtype) for chunk in chunks]
        + [pltpu.VMEM((cols * slots,) + tile, dtype)] * count
        + [pltpu.VMEM((chips * room,) + tile, dtype)] * count
        + [
            pltpu.VMEM((AHEAD, 2 * over, units, cols) + tile, dtype),
            pltpu.VMEM((2, cols, slots) + tile, dtype),
            pltpu.VMEM((2, chips, room) + tile, dtype),
            pltpu.VMEM((2, 2, units, per_group, NARROW, over * LANES), dtype),
            dma((count, 2 * over)), dma((count, 2 * over)),
            dma((count, cols)), dma((count, cols)),
            dma((count, chips)), dma((count, chips)),
            dma((count,)), dma((count, 2)),
            pltpu.VMEM((devices, samples, bag), marked.dtype),
            pltpu.VMEM((devices, samples, bag), marked.dtype),
            pltpu.VMEM((cols, halves, NARROW, table_len), dtype),
            pltpu.VMEM((devices, samples, width), jnp.float32),
            pltpu.VMEM((devices, samples, width), jnp.float32),
            pltpu.VMEM((devices * samples * bag // KEYS, KEYS // bag, KEYS), jnp.float32),
            pltpu.VMEM((devices * samples * bag // KEYS, KEYS, KEYS), jnp.bfloat16),
            pltpu.VMEM((table_len // KEYS // count, devices * samples, KEYS), jnp.bfloat16),
        ]
        + [dma((devices,))] * 4
        + [dma((units,))],
        compiler_params=pltpu.CompilerParams(
            has_side_effects=True, collective_id=number, vmem_limit_bytes=54 * 1024 * 1024
        ),
    )(old_plan, new_plan, view, marked, picks)


def whole_kernel(groups, cols, chunks, old_ref, new_ref, table_ref, ids_ref, out_ref, pooled_ref, *scratch):
    zbufs, spreads, picks = scratch[:chunks], scratch[chunks : 2 * chunks], scratch[2 * chunks : 3 * chunks]
    z_send, z_recv, s_send, s_recv, p_send, p_recv = scratch[3 * chunks : 3 * chunks + 6]
    own_ids, by_slot, tabs, total, sums_ref, source_ref, inverse_ref = scratch[3 * chunks + 6 : 3 * chunks + 13]
    i_send, i_recv, r_send, r_recv, t_sem = scratch[3 * chunks + 13 :]
    g = lax.axis_index("grp")
    c = lax.axis_index("col")
    per_group, narrow, table_len = out_ref.shape
    chunk_rows = table_len // chunks
    sub = chunk_rows // groups

    def aligned(value, unit):
        return pl.multiple_of(value * unit, unit)

    def column_step(k, d):
        to = lax.rem(c + d, cols)
        src = table_ref.at[0, pl.ds(aligned(to, narrow), narrow), pl.ds(k * chunk_rows, chunk_rows)]
        dst = zbufs[k].at[c]
        if d == 0:
            return pltpu.make_async_copy(src, dst, z_recv.at[k, d])
        return pltpu.make_async_remote_copy(
            src, dst, z_send.at[k, d], z_recv.at[k, d], device_id=(g, to), device_id_type=MESH
        )

    def spread_step(k, d):
        to = lax.rem(g + d, groups)
        src = zbufs[k].at[:, :, pl.ds(aligned(to, sub), sub)]
        dst = spreads[k].at[pl.ds(g * cols, cols)]
        if d == 0:
            return pltpu.make_async_copy(src, dst, s_recv.at[k, d])
        return pltpu.make_async_remote_copy(
            src, dst, s_send.at[k, d], s_recv.at[k, d], device_id=(to, c), device_id_type=MESH
        )

    def group_step(k, d):
        to = lax.rem(g + d, groups)
        src = picks[k].at[pl.ds(to * per_group, per_group)]
        dst = out_ref.at[:, :, pl.ds(aligned(k * groups + g, sub), sub)]
        if d == 0:
            return pltpu.make_async_copy(src, dst, p_recv.at[k, d])
        return pltpu.make_async_remote_copy(
            src, dst, p_send.at[k, d], p_recv.at[k, d], device_id=(to, c), device_id_type=MESH
        )

    devices = groups * cols
    me = g * cols + c
    samples, tables, bag = ids_ref.shape

    def ids_step(d):
        to = lax.rem(me + d, devices)
        src, dst = by_slot.at[to], own_ids.at[me]
        if isinstance(d, int):
            return pltpu.make_async_copy(src, dst, i_recv.at[d])
        return pltpu.make_async_remote_copy(
            src, dst, i_send.at[d], i_recv.at[d],
            device_id=(to // cols, lax.rem(to, cols)), device_id_type=MESH,
        )

    def sums_step(d):
        to = lax.rem(me + d, devices)
        src, dst = total.at[to], sums_ref.at[me]
        if isinstance(d, int):
            return pltpu.make_async_copy(src, dst, r_recv.at[d])
        return pltpu.make_async_remote_copy(
            src, dst, r_send.at[d], r_recv.at[d],
            device_id=(to // cols, lax.rem(to, cols)), device_id_type=MESH,
        )

    def each_peer(act):
        def step(d, carry):
            act(d)
            return carry

        lax.fori_loop(1, devices, step, 0)

    def fetch(k):
        return pltpu.make_async_copy(
            table_ref.at[0, :, pl.ds(k * chunk_rows, chunk_rows)], tabs.at[k % 2], t_sem.at[k % 2]
        )

    tile = 512 if chunk_rows % 512 == 0 else 128
    fold = 8 if devices % 8 == 0 else 1

    def pool(k):
        fetch(k).wait()
        if k + 1 < chunks:
            fetch(k + 1).start()
        columns = chunk_rows // tile

        def piece(step, carry):
            block, part = step // columns, lax.rem(step, columns)
            rows = samples * fold
            wanted = own_ids[pl.ds(block * fold, fold)].reshape(rows, bag)
            row = lax.broadcasted_iota(jnp.int32, (rows, tile), 1) + (k * chunk_rows + part * tile)
            counts = jnp.zeros((rows, tile), jnp.float32)
            for i in range(bag):
                counts = jnp.where(wanted[:, i : i + 1] == row, counts + 1.0, counts)
            values = tabs[k % 2, :, pl.ds(aligned(part, tile), tile)]
            sums = lax.dot_general(
                counts.astype(values.dtype), values, (((1,), (1,)), ((), ())),
                preferred_element_type=jnp.float32,
            )
            where = pl.ds(block * fold, fold)
            total[where] = total[where] + sums.reshape(fold, samples, values.shape[0])
            return carry

        lax.fori_loop(0, devices // fold * columns, piece, 0)

    def finish(copy, d):
        if d == 0:
            copy.wait()
        else:
            copy.wait_recv()

    col_order = [d for d in (2, 1, 3) if d < cols] + list(range(4, cols)) + [0]
    grp_order = [d for d in ORDER if d < groups] + list(range(8, groups)) + [0]

    def order_ids(s, carry):
        by_slot[s] = ids_ref[:, pl.ds(old_ref[s], 1), :].reshape(samples, bag)
        return carry

    def locate(j, carry):
        wanted = new_ref[j]

        def look(s, found):
            held = old_ref[s]
            return jnp.where(held == wanted, s, found[0]), jnp.where(held == j, s, found[1])

        source_ref[j], inverse_ref[j] = lax.fori_loop(0, tables, look, (0, 0))
        return carry

    for k in range(min(WINDOW, chunks)):
        for d in col_order:
            column_step(k, d).start()
    fetch(0).start()
    lax.fori_loop(0, tables, order_ids, 0)
    lax.fori_loop(0, tables, locate, 0)
    each_peer(lambda d: ids_step(d).start())
    ids_step(0).start()
    total[...] = jnp.zeros_like(total)
    each_peer(lambda d: ids_step(d).wait_recv())
    ids_step(0).wait()

    def route(k):
        for d in grp_order:
            finish(spread_step(k, d), d)

        def pick(i, carry):
            picks[k][i] = spreads[k][source_ref[i]]
            return carry

        lax.fori_loop(0, groups * per_group, pick, 0)
        for d in grp_order:
            group_step(k, d).start()

    for k in range(chunks):
        for d in col_order:
            finish(column_step(k, d), d)
        for d in grp_order:
            spread_step(k, d).start()
        if k + WINDOW < chunks:
            for d in col_order:
                column_step(k + WINDOW, d).start()
        if k > 0:
            route(k - 1)
        pool(k)
    route(chunks - 1)
    each_peer(lambda d: sums_step(d).start())
    sums_step(0).start()
    for k in range(chunks):
        for d in grp_order:
            finish(group_step(k, d), d)
        for d in col_order:
            if d > 0:
                column_step(k, d).wait_send()
        for d in grp_order:
            if d > 0:
                spread_step(k, d).wait_send()
                group_step(k, d).wait_send()
    each_peer(lambda d: ids_step(d).wait_send())
    each_peer(lambda d: sums_step(d).wait())
    sums_step(0).wait()
    for t in range(tables):
        pooled_ref[:, t, :] = sums_ref[inverse_ref[t]]


def move_whole(old_tables, old_plan, new_plan, marked, groups, cols):
    _, width, table_len = old_tables.shape
    narrow = width // cols
    tables = old_plan.shape[0]
    per_group = tables // groups
    chunks = min(CHUNKS, table_len // (groups * 128))
    chunk_rows = table_len // chunks
    sub = chunk_rows // groups
    dtype = old_tables.dtype
    devices = groups * cols
    samples, _, bag = marked.shape
    sems = [
        pltpu.SemaphoreType.DMA((chunks, n)) for n in (cols, cols, groups, groups, groups, groups)
    ]
    return pl.pallas_call(
        functools.partial(whole_kernel, groups, cols, chunks),
        out_shape=(
            jax.ShapeDtypeStruct((per_group, narrow, table_len), dtype),
            jax.ShapeDtypeStruct((samples, tables, width), jnp.float32),
        ),
        in_specs=[
            pl.BlockSpec(memory_space=pltpu.SMEM),
            pl.BlockSpec(memory_space=pltpu.SMEM),
            pl.BlockSpec(memory_space=pl.ANY),
            pl.BlockSpec(memory_space=pltpu.VMEM),
        ],
        out_specs=(pl.BlockSpec(memory_space=pl.ANY), pl.BlockSpec(memory_space=pltpu.VMEM)),
        scratch_shapes=[pltpu.VMEM((cols, narrow, chunk_rows), dtype)] * chunks
        + [pltpu.VMEM((groups * cols, narrow, sub), dtype)] * chunks
        + [pltpu.VMEM((tables, narrow, sub), dtype)] * chunks
        + sems
        + [
            pltpu.VMEM((devices, samples, bag), marked.dtype),
            pltpu.VMEM((devices, samples, bag), marked.dtype),
            pltpu.VMEM((2, width, chunk_rows), dtype),
            pltpu.VMEM((devices, samples, width), jnp.float32),
            pltpu.VMEM((devices, samples, width), jnp.float32),
            pltpu.SMEM((tables,), jnp.int32),
            pltpu.SMEM((tables,), jnp.int32),
        ]
        + [pltpu.SemaphoreType.DMA((devices,))] * 4
        + [pltpu.SemaphoreType.DMA((2,))],
        compiler_params=pltpu.CompilerParams(
            has_side_effects=True, vmem_limit_bytes=48 * 1024 * 1024
        ),
    )(old_plan, new_plan, old_tables, marked)


def place_kernel(per_group, units, plan_ref, rows_ref, moved_ref, out_ref, zeros, out_sem):
    own = lax.axis_index("grp") * per_group
    zeros[...] = jnp.zeros_like(zeros)

    def used(i):
        return lax.rem(i, units) * UNIT < rows_ref[plan_ref[own + i // units]]

    def window(ref, i):
        return ref.at[i // units, :, pl.ds(pl.multiple_of(lax.rem(i, units) * UNIT, UNIT), UNIT)]

    def store(i, source):
        return pltpu.make_async_copy(source, window(out_ref, i), out_sem.at[i])

    def first(i, carry):
        @pl.when(used(i))
        def _():
            store(i, window(moved_ref, i)).start()

        @pl.when(jnp.logical_not(used(i)))
        def _():
            store(i, zeros).start()

        return carry

    def third(i, carry):
        store(i, zeros).wait()
        return carry

    for step in (first, third):
        lax.fori_loop(0, per_group * units, step, 0)


def clear_unused(moved, new_plan, table_rows):
    per_group, narrow, table_len = moved.shape
    units = table_len // UNIT
    dma = pltpu.SemaphoreType.DMA((per_group * units,))
    return pl.pallas_call(
        functools.partial(place_kernel, per_group, units),
        out_shape=pltpu.HBM(moved.shape, moved.dtype),
        in_specs=[
            pl.BlockSpec(memory_space=pltpu.SMEM),
            pl.BlockSpec(memory_space=pltpu.SMEM),
            pl.BlockSpec(memory_space=pltpu.VMEM),
        ],
        out_specs=pl.BlockSpec(memory_space=pltpu.HBM),
        scratch_shapes=[pltpu.VMEM((narrow, UNIT), moved.dtype), dma],
        compiler_params=pltpu.CompilerParams(vmem_limit_bytes=12 * 1024 * 1024),
    )(new_plan, table_rows, moved)


def vmem_bytes(chunks, units, cols, chips, samples, bag, caps):
    slots, room = caps
    tiles = sum(2 * chunk[1] * units * cols + cols * slots + chips * room for chunk in chunks)
    tiles += 2 * (AHEAD * chunks[0][1] * units * cols + cols * slots + chips * room) + 3 * 1024
    counts = KEYS * (samples * bag + units * UNIT // KEYS // len(chunks) * samples)
    return (tiles * NARROW * LANES + counts) * 2


def body(old_tables, table_rows, old_plan, new_plan, ids, bag_len):
    groups = lax.axis_size("grp")
    cols = lax.axis_size("col")
    tables = old_plan.shape[0]
    per_group = tables // groups
    _, width, table_len = old_tables.shape
    units = table_len // UNIT
    chips = groups // 2
    bag_iota = lax.broadcasted_iota(jnp.int32, (1, 1, ids.shape[2]), 2)
    marked = lax.optimization_barrier(jnp.where(bag_iota < bag_len[:, :, None], ids, -1))
    chunks = chunk_list(UNIT, width // cols // NARROW)

    over = chunks[0][1]
    slot = jnp.arange(tables, dtype=jnp.int32)
    plane, group = slot % cols, slot // cols
    part, base = (group // 2) % over, group // 2 // over
    order = group % 2 * over + part
    held = jnp.sum(jnp.where(old_plan[:, None] == slot[None, :], table_rows[None, :], 0), axis=1) // UNIT
    position = jnp.sum(jnp.where(old_plan[:, None] == new_plan[None, :], slot[None, :], 0), axis=1)
    target = position // per_group // 2
    slot_of = jnp.sum(jnp.where(old_plan[None, :] == slot[:, None], slot[None, :], 0), axis=1)
    same = base[:, None] == base[None, :]
    same_plane = plane[:, None] == plane[None, :]
    first = order[None, :] < order[:, None]
    z_off = jnp.sum(jnp.where(same & same_plane & first, held[None, :], 0), axis=1)
    ahead = (plane[None, :] < plane[:, None]) | (same_plane & first)
    c_off = jnp.sum(jnp.where(same & (target[:, None] == target[None, :]) & ahead, held[None, :], 0), axis=1)
    z_need, c_need = z_off + held, c_off + held

    g = lax.axis_index("grp")
    c = lax.axis_index("col")
    chip = g // 2

    def variant(number, caps):
        slots, room = caps

        def run(old_tables, table_rows, old_plan, new_plan, marked):
            mine = base == chip // over
            n = jnp.arange(slots, dtype=jnp.int32)[:, None]
            inside = (mine & (plane == c))[None, :] & (n >= z_off[None, :]) & (n < (z_off + held)[None, :])
            z_pick = jnp.sum(jnp.where(inside, (order * units - z_off)[None, :] + n, 0), axis=1)
            m = jnp.arange(chips * room, dtype=jnp.int32)[:, None]
            to, m = (chip + m // room) % chips, m % room
            inside = mine[None, :] & (target[None, :] == to) & (m >= c_off[None, :]) & (m < (c_off + held)[None, :])
            c_pick = jnp.sum(jnp.where(inside, (plane * slots + z_off - c_off)[None, :] + m, 0), axis=1)
            f = jnp.arange(2 * per_group * units, dtype=jnp.int32)[:, None]
            where, e = chip * 2 * per_group + f // units, f % units
            inside = (position[None, :] == where) & (e < held[None, :])
            f_pick = jnp.sum(jnp.where(inside, (base * over * room + c_off)[None, :] + e, 0), axis=1)
            picks = jnp.concatenate([z_pick, c_pick, f_pick, slot_of])
            moved, pooled = move_tables(
                old_tables, old_plan, new_plan, marked, picks, groups, cols, chunks, caps, number
            )
            return clear_unused(moved, new_plan, table_rows), pooled

        return run

    full = 2 * over * units
    room_full = 2 * per_group * units
    caps = [(full * a // 64, room_full * b // 64) for a, b in SHARES]
    caps = [cap for cap in caps if vmem_bytes(chunks, units, cols, chips, ids.shape[0] * groups * cols, ids.shape[2], cap) < VMEM_ROOM]
    branches = [variant(number, cap) for number, cap in enumerate(caps)]
    if not caps or caps[-1][0] < full:

        def fallback(old_tables, table_rows, old_plan, new_plan, marked):
            moved, pooled = move_whole(old_tables, old_plan, new_plan, marked, groups, cols)
            return clear_unused(moved, new_plan, table_rows), pooled

        branches.append(fallback)
    misfits = (((z_need > cap[0]) | (c_need > cap[1])).astype(jnp.int32) for cap in caps[: len(branches) - 1])
    level = jnp.max(sum(misfits, start=jnp.zeros_like(z_need)))
    return lax.switch(level, branches, old_tables, table_rows, old_plan, new_plan, marked)


def solution(mesh):
    return jax.shard_map(
        body,
        mesh=mesh,
        in_specs=(
            P(("grp", "col"), None, None),
            P(),
            P(),
            P(),
            P(("grp", "col"), None, None),
            P(("grp", "col"), None),
        ),
        out_specs=(P("grp", "col", None), P(("grp", "col"), None, None)),
        check_vma=False,
    )
```
